128 devices in a mesh: section: 8 (over x, y_lo), seq: 16 (over z, y_hi, core).
Axes of the slice: x: 4, y: 4 (y_hi: 2, y_lo: 2; y = y_hi * 2 + y_lo), z: 4, core: 2. Of those that a mesh axis runs over, the one named last changes fastest.
Arguments:
- queries: bfloat16 [8, 2048, 4096], P('section', 'seq'), may hold values from -500 to 500
- keys: bfloat16 [8, 2048, 512], P('section', 'seq'), may hold values from -6 to 6
- values: bfloat16 [8, 2048, 512], P('section', 'seq'), may hold values from -6 to 6
- out_grad: bfloat16 [8, 2048, 4096], P('section', 'seq'), may hold values from -6 to 6
- documents: int32 [8, 2048], P('section'), may hold values from 0 to 3, never falling along the last dimension, each value on 1 to 1024 neighbouring positions
- query_weight: bfloat16 [8, 4096, 4096], P('section', 'seq'), may hold values from -0.09375 to 0.09375
- key_weight: bfloat16 [8, 512, 4096], P('section'), may hold values from -0.125 to 0.125
- value_weight: bfloat16 [8, 512, 4096], P('section'), may hold values from -0.125 to 0.125
Outputs:
- upstream: bfloat16 [8, 2048, 4096], P('section', 'seq')
The draws below stay inside these ranges and needn't reach their ends.
Inputs may be any that keep to these rules, and one draw needn't show every extreme that they name: `documents`: each section's document ids never fall along its tokens.
All inputs are finite; a program needn't handle non-finite values.
Results may differ from the reference program's by a relative error of at most 0.0058.
Values may be sent and summed in bfloat16 or wider, within the bound.
A program may use at most 192 MiB of HBM per device.

```python
import math
import jax
import jax.numpy as jnp
import numpy as np
from jax import lax

D = 4096
H = 32
KV = 4
HD = 128
SECTIONS = 8
TOKENS = 2048
N_SEQ = 16


def query_key_pair(key):
    base = jax.random.fold_in(key, 11)
    key_q, key_k = jax.random.split(base, 2)
    queries = jax.random.normal(key_q, (SECTIONS, TOKENS, H * HD), jnp.float32)
    keys = jax.random.normal(key_k, (SECTIONS, TOKENS, KV * HD), jnp.float32)
    keys = jnp.clip(keys, -6.0, 6.0)
    return (queries, keys)


def draw_queries(key, part):
    return query_key_pair(key)[0].astype(jnp.bfloat16)


def draw_keys(key, part):
    return query_key_pair(key)[1].astype(jnp.bfloat16)


def shard_levels(rng, shape, shards, least, top_value):
    def one(axis_at, parts):
        draws = jax.random.uniform(jax.random.fold_in(jax.random.fold_in(rng, 6), axis_at), (parts,), jnp.float32, least / len(shards), top_value / len(shards))
        return jnp.repeat(jnp.exp(draws), shape[axis_at] // parts).reshape((-1,) + (1,) * (len(shape) - axis_at - 1))

    loudness = one(*shards[0])
    for cut in shards[1:]:
        loudness = loudness * one(*cut)
    return loudness


def split_up(amount, total, most, slope):
    weights = [(1 << 20) // math.isqrt(rank ** slope) + 1 for rank in range(2, amount + 1)]
    rest, counts = total - most - (amount - 1), [1] * (amount - 1)
    while rest > 0:
        movable = [i for i in range(amount - 1) if counts[i] < most]
        pool, remaining = sum([weights[i] for i in movable]), rest
        for i in movable:
            extra = min(most - counts[i], max(1, remaining * weights[i] // pool), rest)
            counts[i] = counts[i] + extra
            rest = rest - extra
    return np.array([most] + counts)


def ragged(own_key, amount, total, bound, slope):
    if amount == 2:
        one = jax.random.randint(own_key, (), max(1, total - bound), min(bound, total - 1) + 1)
        return jnp.stack([one, total - one])
    tallies = jnp.asarray(split_up(amount, total, bound, slope), jnp.int32)
    twos = (amount - 1) // 2
    donor, taker = tallies[1:1 + 2 * twos:2], tallies[2:2 + 2 * twos:2]
    slack = jnp.minimum(donor - 1, bound - taker)
    passed = jax.random.randint(jax.random.fold_in(own_key, 1), (twos,), 0, 1 << 20) % (slack + 1)
    tallies = tallies.at[1:1 + 2 * twos:2].set(donor - passed).at[2:2 + 2 * twos:2].set(taker + passed)
    return tallies[jax.random.permutation(jax.random.fold_in(own_key, 2), amount)]


def normal_values(key, dims, deviation, reach, cuts=(), kind=jnp.bfloat16):
    loudness = shard_levels(key, dims, cuts, -0.22, 0.18) if cuts else 1.0
    array = jax.random.normal(key, dims, jnp.float32) * deviation * loudness
    return jnp.minimum(jnp.maximum(array, -reach), reach).astype(kind)


def setup_inputs(seed: int = 0) -> dict:
    streams_of = jax.random.split(jax.random.key(seed), 9)
    return {
        "queries": draw_queries(jax.random.fold_in(streams_of[8], 71), 0),
        "keys": draw_keys(jax.random.fold_in(streams_of[8], 71), 0),
        "values": normal_values(streams_of[2], (SECTIONS, TOKENS, KV * HD), 1.0, 6.0, ((0, 8), (1, 16))),
        "out_grad": normal_values(streams_of[3], (SECTIONS, TOKENS, H * HD), 1.0, 6.0, ((0, 8), (1, 16))),
        "documents": jax.vmap(lambda own: jnp.searchsorted(jnp.cumsum(ragged(own, 4, TOKENS, TOKENS // 2, 0)), jnp.arange(TOKENS), side="right"))(jax.random.split(streams_of[4], SECTIONS)).reshape((SECTIONS, TOKENS)).astype(jnp.int32),
        "query_weight": normal_values(streams_of[5], (SECTIONS, H * HD, D), (H * HD) ** -0.5, 0.09375, ((0, 8), (1, 16))),
        "key_weight": normal_values(streams_of[6], (SECTIONS, KV * HD, D), (N_SEQ * HD) ** -0.5, 0.125, ((0, 8),)),
        "value_weight": normal_values(streams_of[7], (SECTIONS, KV * HD, D), (N_SEQ * HD) ** -0.5, 0.125, ((0, 8),)),
    }


def slot_grads(index, q_all, k_all, v_all, o_all, ids):
    per = H // N_SEQ
    total = q_all.shape[0]
    kvh = index * KV // N_SEQ
    scale = 1.0 / math.sqrt(HD)
    q_blk = lax.dynamic_slice_in_dim(q_all, index * per * HD, per * HD, 1).reshape(total, per, HD).astype(jnp.float32)
    o_blk = lax.dynamic_slice_in_dim(o_all, index * per * HD, per * HD, 1).reshape(total, per, HD).astype(jnp.float32)
    k_head = lax.dynamic_slice_in_dim(k_all, kvh * HD, HD, 1).astype(jnp.float32)
    v_head = lax.dynamic_slice_in_dim(v_all, kvh * HD, HD, 1).astype(jnp.float32)
    rows = lax.iota(jnp.int32, total)
    allowed = (rows[None, :] <= rows[:, None]) & (ids[None, :] == ids[:, None])
    scores = jnp.einsum('bhd,td->hbt', q_blk, k_head) * scale
    scores = jnp.where(allowed[None], scores, -jnp.inf)
    top = lax.optimization_barrier(jnp.max(scores, axis=-1, keepdims=True))
    expo = jnp.exp(scores - top)
    prob = expo / lax.optimization_barrier(jnp.sum(expo, axis=-1, keepdims=True))
    prob_low = prob.astype(jnp.bfloat16)
    dprob = jnp.einsum('bhd,td->hbt', o_blk, v_head)
    delta = lax.optimization_barrier(jnp.sum(prob * dprob, axis=-1, keepdims=True))
    dscore = (prob * (dprob - delta) * scale).astype(jnp.bfloat16).astype(jnp.float32)
    dquery = jnp.einsum('hbt,td->bhd', dscore, k_head).astype(jnp.bfloat16).reshape(total, per * HD)
    dkey = jnp.einsum('hbt,bhd->td', dscore, q_blk).astype(jnp.bfloat16)
    dvalue = jnp.einsum('hbt,bhd->td', prob_low.astype(jnp.float32), o_blk).astype(jnp.bfloat16)
    return (dquery, dkey, dvalue)

def reference(queries, keys, values, out_grad, documents, query_weight, key_weight, value_weight):
    reps = N_SEQ // KV
    grads = []
    for section in range(SECTIONS):

        def one_slot(index):
            return slot_grads(index, queries[section], keys[section], values[section], out_grad[section], documents[section])
        dq_s, dk_s, dv_s = lax.map(one_slot, jnp.arange(N_SEQ, dtype=jnp.int32))
        total = queries.shape[1]
        dquery = jnp.transpose(dq_s, (1, 0, 2)).reshape(total, H * HD)
        dkey = jnp.transpose(dk_s, (1, 0, 2)).reshape(total, N_SEQ * HD)
        dvalue = jnp.transpose(dv_s, (1, 0, 2)).reshape(total, N_SEQ * HD)
        wk_rep = jnp.repeat(key_weight[section].reshape(KV, HD, D), reps, axis=0).reshape(N_SEQ * HD, D)
        wv_rep = jnp.repeat(value_weight[section].reshape(KV, HD, D), reps, axis=0).reshape(N_SEQ * HD, D)
        dinput = jnp.dot(dquery, query_weight[section], preferred_element_type=jnp.float32)
        dinput = dinput + jnp.dot(dkey, wk_rep, preferred_element_type=jnp.float32)
        dinput = dinput + jnp.dot(dvalue, wv_rep, preferred_element_type=jnp.float32)
        grads.append(dinput.astype(jnp.bfloat16))
    grads = grads[1:] + [jnp.zeros_like(grads[0])]
    return jnp.stack(grads, axis=0)
```

```python
import math

import jax
import jax.numpy as jnp
from jax import lax
from jax.experimental import pallas as pl
from jax.experimental.pallas import tpu as pltpu
from jax.sharding import PartitionSpec as P

HD = 128
ROWS = 128
GW = 1024
D = 4096
NC = 8
CW = D // NC
WIN = 9
SCALE = 1.0 / math.sqrt(HD)
NEG = -1e30
MESH = pl.DeviceIdType.MESH
F32 = jnp.float32
BF16 = jnp.bfloat16


def remote(src, dst, send, recv, device):
    return pltpu.make_async_remote_copy(
        src_ref=src, dst_ref=dst, send_sem=send, recv_sem=recv, device_id=device, device_id_type=MESH
    )


def kernel(
    q_ref, k_ref, v_ref, o_ref, doc_ref, w_ref, wk_ref, wv_ref,
    out_ref,
    qs, os_, kv, start, p_s, ds_s, dk, dv, dq, w8, wkv, stage, recv, part, own,
    dkv_s, dkv_c, dkv_o, dkv_i, fin,
    loc, kvz_s, kvz_r, kvy_s, kvy_r, kvc_s, kvc_r, qo_s, qo_r,
    wy_s, wy_r, wc_s, wc_r, wf_s, wf_r, rs_s, rs_r, dc_s, dc_r, dd_s, dd_r, hop_s, hop_r,
):
    sec = lax.axis_index("section")
    seq = lax.axis_index("seq")
    z = seq // 4
    y = lax.rem(seq // 2, 2)
    c = lax.rem(seq, 2)
    yc = y * 2 + c

    def dev(zz, yy, cc):
        return (sec, zz * 4 + yy * 2 + cc)

    def zoff(d):
        return lax.rem(z + d, 4)

    core = dev(z, y, 1 - c)
    ypart = dev(z, 1 - y, c)

    own_q = pltpu.make_async_copy(q_ref.at[:, pl.ds(pl.multiple_of(z * GW, GW), GW)], qs.at[z], loc.at[0])
    own_o = pltpu.make_async_copy(o_ref.at[:, pl.ds(pl.multiple_of(z * GW, GW), GW)], os_.at[z], loc.at[1])
    own_k = pltpu.make_async_copy(
        k_ref.at[:, pl.ds(pl.multiple_of(z * HD, HD), HD)], kv.at[z + 2, yc, :, 0:HD], loc.at[2]
    )
    own_v = pltpu.make_async_copy(
        v_ref.at[:, pl.ds(pl.multiple_of(z * HD, HD), HD)], kv.at[z + 2, yc, :, HD : 2 * HD], loc.at[3]
    )
    own_w = pltpu.make_async_copy(w_ref, w8.at[yc], loc.at[4])
    own_wk = pltpu.make_async_copy(wk_ref, wkv.at[:, 0], loc.at[5])
    own_wv = pltpu.make_async_copy(wv_ref, wkv.at[:, 1], loc.at[6])
    for copy in (own_k, own_v, own_q, own_o, own_w, own_wk, own_wv):
        copy.start()

    barrier = pltpu.get_barrier_semaphore()
    for dy in range(2):
        for dz in range(4):
            if dy or dz:
                pl.semaphore_signal(
                    barrier, inc=1, device_id=dev(zoff(dz), lax.rem(y + dy, 2), c), device_id_type=MESH
                )
    pl.semaphore_signal(barrier, inc=1, device_id=core, device_id_type=MESH)

    @pl.when(sec > 0)
    def _():
        pl.semaphore_signal(barrier, inc=1, device_id=(sec - 1, seq), device_id_type=MESH)

    @pl.when(sec < 7)
    def _():
        pl.semaphore_signal(barrier, inc=1, device_id=(sec + 1, seq), device_id_type=MESH)

    pl.semaphore_wait(barrier, 8 + jnp.where(sec > 0, 1, 0) + jnp.where(sec < 7, 1, 0))

    kv_copies = []
    for d in (1, 3, 2):
        zd = zoff(d)
        cols = pl.ds(pl.multiple_of(zd * HD, HD), HD)
        kv_copies.append(
            (
                remote(k_ref.at[:, cols], kv.at[z + 2, yc, :, 0:HD], kvz_s.at[0, d], kvz_r.at[0, d], dev(zd, y, c)),
                remote(
                    v_ref.at[:, cols], kv.at[z + 2, yc, :, HD : 2 * HD], kvz_s.at[1, d], kvz_r.at[1, d], dev(zd, y, c)
                ),
            )
        )
    for pair in kv_copies:
        pair[0].start()
        pair[1].start()

    def w_y(n):
        cols = pl.ds(n * CW, CW)
        return remote(w_ref.at[:, cols], w8.at[yc, :, cols], wy_s.at[n], wy_r.at[n], ypart)

    def w_y_in(n):
        cols = pl.ds(n * CW, CW)
        at = (1 - y) * 2 + c
        return remote(w_ref.at[:, cols], w8.at[at, :, cols], wy_s.at[n], wy_r.at[n], ypart)

    w_core = remote(w_ref, w8.at[yc], wc_s.at[0], wc_r.at[0], core)

    def w_fwd(n):
        cols = pl.ds(n * CW, CW)
        at = (1 - y) * 2 + c
        return remote(w8.at[at, :, cols], w8.at[at, :, cols], wf_s.at[n], wf_r.at[n], core)

    def w_fwd_in(n):
        cols = pl.ds(n * CW, CW)
        at = (1 - y) * 2 + 1 - c
        return remote(w8.at[at, :, cols], w8.at[at, :, cols], wf_s.at[n], wf_r.at[n], core)

    w_y(0).start()
    qo_copies = []
    for d in (2, 1, 3):
        zd = zoff(d)
        cols = pl.ds(pl.multiple_of(zd * GW, GW), GW)
        qo_copies.append(remote(q_ref.at[:, cols], qs.at[z], qo_s.at[0, d], qo_r.at[0, d], dev(zd, y, c)))
        qo_copies.append(remote(o_ref.at[:, cols], os_.at[z], qo_s.at[1, d], qo_r.at[1, d], dev(zd, y, c)))
    for copy in qo_copies:
        copy.start()
    w_core.start()

    doc = doc_ref[...]
    first = jnp.zeros_like(doc)
    for value in (1, 2, 3):
        before = jnp.sum((doc < value).astype(F32), axis=1, keepdims=True).astype(jnp.int32)
        first = jnp.where(doc == value, before, first)
    start[...] = first
    kv[0:2] = jnp.zeros((2, 4, ROWS, 2 * HD), BF16)
    dk[...] = jnp.zeros_like(dk)
    dv[...] = jnp.zeros_like(dv)

    own_k.wait()
    own_v.wait()
    for d in (1, 3, 2):
        zs = lax.rem(z + 4 - d, 4)
        remote(k_ref.at[:, 0:HD], kv.at[zs + 2, yc, :, 0:HD], kvz_s.at[0, d], kvz_r.at[0, d], core).wait_recv()
        remote(
            v_ref.at[:, 0:HD], kv.at[zs + 2, yc, :, HD : 2 * HD], kvz_s.at[1, d], kvz_r.at[1, d], core
        ).wait_recv()
    kv_y = remote(kv.at[2:6, yc], kv.at[2:6, yc], kvy_s.at[0], kvy_r.at[0], ypart)
    kv_y.start()
    kv_c0 = remote(kv.at[2:6, yc], kv.at[2:6, yc], kvc_s.at[0], kvc_r.at[0], core)
    kv_c0.start()
    for n in range(1, NC):
        w_y(n).start()
    at = (1 - y) * 2 + c
    remote(kv.at[2:6, at], kv.at[2:6, at], kvy_s.at[0], kvy_r.at[0], ypart).wait_recv()
    kv_c1 = remote(kv.at[2:6, at], kv.at[2:6, at], kvc_s.at[1], kvc_r.at[1], core)
    kv_c1.start()
    at = y * 2 + 1 - c
    remote(kv.at[2:6, at], kv.at[2:6, at], kvc_s.at[0], kvc_r.at[0], core).wait_recv()
    at = (1 - y) * 2 + 1 - c
    remote(kv.at[2:6, at], kv.at[2:6, at], kvc_s.at[1], kvc_r.at[1], core).wait_recv()

    kv_rows = kv.reshape(24 * ROWS, 2 * HD)

    def attend(i, carry):
        d = lax.rem(i, 2) * 2 + i // 2
        zb = lax.rem(z + 4 - d, 4)

        @pl.when(d == 0)
        def _():
            own_q.wait()
            own_o.wait()

        @pl.when(d > 0)
        def _():
            remote(q_ref.at[:, 0:GW], qs.at[zb], qo_s.at[0, d], qo_r.at[0, d], core).wait_recv()
            remote(o_ref.at[:, 0:GW], os_.at[zb], qo_s.at[1, d], qo_r.at[1, d], core).wait_recv()

        block = zb * 4 + yc
        at = pl.multiple_of(block * ROWS, ROWS)
        k_win = kv_rows[pl.ds(at, WIN * ROWS), 0:HD]
        base = (block - 8) * ROWS
        lower = start[:, pl.ds(at, ROWS)] - base
        lower = jnp.concatenate([lower, lower], axis=1)

        def heads(hp, carry):
            cols = pl.ds(pl.multiple_of(hp * 2 * HD, 2 * HD), 2 * HD)
            q2 = qs[zb, :, cols]
            q2 = jnp.concatenate([q2[:, 0:HD], q2[:, HD:]], axis=0)
            o2 = os_[zb, :, cols]
            o2 = jnp.concatenate([o2[:, 0:HD], o2[:, HD:]], axis=0)
            v_win = kv_rows[pl.ds(at, WIN * ROWS), HD : 2 * HD]
            k_win = kv_rows[pl.ds(at, WIN * ROWS), 0:HD]
            nt = (((1,), (1,)), ((), ()))
            s = lax.dot_general(k_win, q2, nt, preferred_element_type=F32)
            key = lax.broadcasted_iota(jnp.int32, (8 * ROWS, 2 * ROWS), 0)
            s_a = jnp.where(key >= lower, s[: 8 * ROWS], NEG)
            key = lax.broadcasted_iota(jnp.int32, (ROWS, 2 * ROWS), 0)
            row = lax.broadcasted_iota(jnp.int32, (ROWS, 2 * ROWS), 1)
            row = jnp.where(row >= ROWS, row - ROWS, row)
            s_b = jnp.where((key + 8 * ROWS >= lower) & (key <= row), s[8 * ROWS :], NEG)
            s = jnp.concatenate([s_a, s_b], axis=0)
            top = jnp.max(s, axis=0, keepdims=True)
            e = jnp.exp2((s - top) * (SCALE * math.log2(math.e)))
            inv = 1.0 / jnp.sum(e, axis=0, keepdims=True)
            dp = lax.dot_general(v_win, o2, nt, preferred_element_type=F32)
            delta = jnp.sum(e * dp, axis=0, keepdims=True) * inv
            p_s[:, cols] = (e * inv).astype(BF16)
            ds_s[:, cols] = (e * (dp - delta) * (inv * SCALE)).astype(BF16)
            return carry

        lax.fori_loop(0, 4, heads, 0)
        qb = qs[zb]
        ob = os_[zb]
        qb = jnp.concatenate([qb[:, h * HD : (h + 1) * HD] for h in range(8)], axis=0)
        ob = jnp.concatenate([ob[:, h * HD : (h + 1) * HD] for h in range(8)], axis=0)
        win = pl.ds(at, WIN * ROWS)
        dv[win, :] += jnp.dot(p_s[...], ob, preferred_element_type=F32)
        dk[win, :] += jnp.dot(ds_s[...], qb, preferred_element_type=F32)
        dqt = lax.dot_general(k_win, ds_s[...], (((0,), (0,)), ((), ())), preferred_element_type=F32)
        for h in range(8):
            dq[pl.ds(pl.multiple_of(zb * ROWS, ROWS), ROWS), h * HD : (h + 1) * HD] = dqt[
                :, h * HD : (h + 1) * HD
            ].T.astype(BF16)
        return carry

    lax.fori_loop(0, 4, attend, 0)

    def blocks(b, carry):
        rows = pl.ds(pl.multiple_of((b + 8) * ROWS, ROWS), ROWS)
        dkv_s[b // 4, lax.rem(b, 4), :, 0:HD] = dk[rows, :].astype(BF16)
        dkv_s[b // 4, lax.rem(b, 4), :, HD : 2 * HD] = dv[rows, :].astype(BF16)
        return carry

    lax.fori_loop(0, 16, blocks, 0)
    dc_copies = [
        remote(dkv_s.at[:, yy * 2 + 1 - c], dkv_c.at[yy], dc_s.at[yy], dc_r.at[yy], core) for yy in range(2)
    ]
    for copy in dc_copies:
        copy.start()

    own_w.wait()
    w_core.wait()

    def rs(n, d):
        zd = zoff(d)
        return remote(stage.at[zd, n], recv.at[d - 1, n], rs_s.at[d - 1, n], rs_r.at[d - 1, n], dev(zd, y, c))

    w_y_in(0).wait_recv()
    w_fwd(0).start()

    def product(n, carry):
        cols = pl.ds(pl.multiple_of(n * CW, CW), CW)

        @pl.when(n < NC - 1)
        def _():
            w_y_in(n + 1).wait_recv()
            w_fwd(n + 1).start()

        w_fwd_in(n).wait_recv()
        part[...] = jnp.dot(dq[...], w8.reshape(GW, D)[:, cols], preferred_element_type=F32)
        for zd in range(4):
            stage[zd, n] = part[zd * ROWS : (zd + 1) * ROWS, :].astype(BF16)
        own[:, cols] = part[pl.ds(pl.multiple_of(z * ROWS, ROWS), ROWS), :]
        for d in (2, 1, 3):
            rs(n, d).start()
        return carry

    def dkv_sum():
        for yy in range(2):
            dc_copies[yy].wait_recv()

            def add(zz, carry):
                rows = pl.ds(pl.multiple_of((zz * 4 + yy * 2 + c + 8) * ROWS, ROWS), ROWS)
                dkv_o[yy, zz, :, 0:HD] = (dk[rows, :] + dkv_c[yy, zz, :, 0:HD].astype(F32)).astype(BF16)
                dkv_o[yy, zz, :, HD : 2 * HD] = (dv[rows, :] + dkv_c[yy, zz, :, HD : 2 * HD].astype(F32)).astype(BF16)
                return carry

            lax.fori_loop(0, 4, add, 0)

    def dd(dy, dz):
        yy = lax.rem(y + dy, 2)
        zz = zoff(dz)
        return remote(dkv_o.at[yy, zz], dkv_i.at[y, z], dd_s.at[dy, dz], dd_r.at[dy, dz], dev(zz, yy, c))

    dkv_sum()
    for dy in range(2):
        for dz in range(4):
            if dy or dz:
                dd(dy, dz).start()
    dkv_i[y, z] = dkv_o[y, z]
    lax.fori_loop(0, NC, product, 0)
    own_wk.wait()
    own_wv.wait()
    for dy in range(2):
        for dz in range(4):
            if dy or dz:
                ys = lax.rem(y + dy, 2)
                zs = lax.rem(z + 4 - dz, 4)
                remote(
                    dkv_o.at[ys, zs], dkv_i.at[ys, zs], dd_s.at[dy, dz], dd_r.at[dy, dz], core
                ).wait_recv()

    def hop(n):
        cols = pl.ds(n * CW, CW)
        return remote(fin.at[:, cols], out_ref.at[:, cols], hop_s.at[n], hop_r.at[n], (jnp.maximum(sec - 1, 0), seq))

    def finish(n, carry):
        cols = pl.ds(pl.multiple_of(n * CW, CW), CW)
        dkv = jnp.concatenate(
            [(dkv_i[0, zz].astype(F32) + dkv_i[1, zz].astype(F32)).astype(BF16) for zz in range(4)], axis=1
        )
        total = own[:, cols] + jnp.dot(dkv, wkv.reshape(GW, D)[:, cols], preferred_element_type=F32)
        for d in (1, 3, 2):
            rs(n, d).wait_recv()
            total = total + recv[d - 1, n].astype(F32)
        fin[:, cols] = total.astype(BF16)

        @pl.when(sec > 0)
        def _():
            hop(n).start()

        return carry

    lax.fori_loop(0, NC, finish, 0)

    @pl.when(sec == 7)
    def _():
        out_ref[...] = jnp.zeros_like(out_ref)

    for pair in kv_copies:
        pair[0].wait_send()
        pair[1].wait_send()
    for copy in qo_copies + [kv_y, kv_c0, kv_c1] + dc_copies:
        copy.wait_send()
    for dy in range(2):
        for dz in range(4):
            if dy or dz:
                dd(dy, dz).wait_send()

    def drain(n, carry):
        w_y(n).wait_send()
        w_fwd(n).wait_send()
        for d in (1, 2, 3):
            rs(n, d).wait_send()

        @pl.when(sec > 0)
        def _():
            hop(n).wait_send()

        @pl.when(sec < 7)
        def _():
            hop(n).wait_recv()

        return carry

    lax.fori_loop(0, NC, drain, 0)


def body(queries, keys, values, out_grad, documents, query_weight, key_weight, value_weight):
    hbm = pl.BlockSpec(memory_space=pltpu.MemorySpace.HBM)
    vmem = pl.BlockSpec(memory_space=pltpu.VMEM)
    dma = pltpu.SemaphoreType.DMA
    scratch = [
        pltpu.VMEM((4, ROWS, GW), BF16),
        pltpu.VMEM((4, ROWS, GW), BF16),
        pltpu.VMEM((6, 4, ROWS, 2 * HD), BF16),
        pltpu.VMEM((1, 2048), jnp.int32),
        pltpu.VMEM((WIN * ROWS, GW), BF16),
        pltpu.VMEM((WIN * ROWS, GW), BF16),
        pltpu.VMEM((24 * ROWS, HD), F32),
        pltpu.VMEM((24 * ROWS, HD), F32),
        pltpu.VMEM((4 * ROWS, GW), BF16),
        pltpu.VMEM((4, 256, D), BF16),
        pltpu.VMEM((4, 2, HD, D), BF16),
        pltpu.VMEM((4, NC, ROWS, CW), BF16),
        pltpu.VMEM((3, NC, ROWS, CW), BF16),
        pltpu.VMEM((4 * ROWS, CW), F32),
        pltpu.VMEM((ROWS, D), F32),
        pltpu.VMEM((4, 4, ROWS, 2 * HD), BF16),
        pltpu.VMEM((2, 4, ROWS, 2 * HD), BF16),
        pltpu.VMEM((2, 4, ROWS, 2 * HD), BF16),
        pltpu.VMEM((2, 4, ROWS, 2 * HD), BF16),
        pltpu.VMEM((ROWS, D), BF16),
        dma((7,)),
        dma((2, 4)), dma((2, 4)),
        dma((1,)), dma((1,)),
        dma((2,)), dma((2,)),
        dma((2, 4)), dma((2, 4)),
        dma((NC,)), dma((NC,)),
        dma((1,)), dma((1,)),
        dma((NC,)), dma((NC,)),
        dma((3, NC)), dma((3, NC)),
        dma((2,)), dma((2,)),
        dma((2, 4)), dma((2, 4)),
        dma((NC,)), dma((NC,)),
    ]
    out = pl.pallas_call(
        kernel,
        out_shape=jax.ShapeDtypeStruct((ROWS, D), BF16),
        in_specs=[hbm, hbm, hbm, hbm, vmem, hbm, hbm, hbm],
        out_specs=vmem,
        scratch_shapes=scratch,
        compiler_params=pltpu.CompilerParams(
            collective_id=0, has_side_effects=True, vmem_limit_bytes=67043328
        ),
    )(
        queries[0],
        keys[0],
        values[0],
        out_grad[0],
        documents,
        query_weight[0],
        key_weight[0].reshape(4, HD, D),
        value_weight[0].reshape(4, HD, D),
    )
    return out[None]


def solution(mesh):
    in_specs = (
        P("section", "seq", None),
        P("section", "seq", None),
        P("section", "seq", None),
        P("section", "seq", None),
        P("section", None),
        P("section", "seq", None),
        P("section", None, None),
        P("section", None, None),
    )
    out_specs = P("section", "seq", None)
    return jax.shard_map(body, mesh=mesh, in_specs=in_specs, out_specs=out_specs, check_vma=False)
```

```python
import math

import jax
import jax.numpy as jnp
from jax import lax
from jax.experimental import pallas as pl
from jax.experimental.pallas import tpu as pltpu
from jax.sharding import PartitionSpec as P

HD = 128
ROWS = 128
GW = 1024
D = 4096
NC = 8
CW = D // NC
W_EARLY = 6
LAG = 4
WIN = 9
SCALE = 1.0 / math.sqrt(HD)
NEG = -1e30
MESH = pl.DeviceIdType.MESH
F32 = jnp.float32
BF16 = jnp.bfloat16


def remote(src, dst, send, recv, device):
    return pltpu.make_async_remote_copy(
        src_ref=src, dst_ref=dst, send_sem=send, recv_sem=recv, device_id=device, device_id_type=MESH
    )


def kernel(
    q_ref, k_ref, v_ref, o_ref, doc_ref, w_ref, wk_ref, wv_ref,
    out_ref,
    qs, os_, kv, start, p_s, ds_s, dk, dv, dq, w8, wkv, half_s, half_r, full_s, full_r, part, own,
    dkv_s, dkv_c, dkv_o, dkv_i, fin,
    loc, kvz_s, kvz_r, kvy_s, kvy_r, kvc_s, kvc_r, qo_s, qo_r,
    wy_s, wy_r, wc_s, wc_r, wf_s, wf_r, ra_s, ra_r, rb_s, rb_r, dc_s, dc_r, dd_s, dd_r, hop_s, hop_r,
):
    sec = lax.axis_index("section")
    seq = lax.axis_index("seq")
    z = seq // 4
    y = lax.rem(seq // 2, 2)
    c = lax.rem(seq, 2)
    yc = y * 2 + c

    def dev(zz, yy, cc):
        return (sec, zz * 4 + yy * 2 + cc)

    def zoff(d):
        return lax.rem(z + d, 4)

    core = dev(z, y, 1 - c)
    ypart = dev(z, 1 - y, c)

    own_q = pltpu.make_async_copy(q_ref.at[:, pl.ds(pl.multiple_of(z * GW, GW), GW)], qs.at[z], loc.at[0])
    own_o = pltpu.make_async_copy(o_ref.at[:, pl.ds(pl.multiple_of(z * GW, GW), GW)], os_.at[z], loc.at[1])
    own_k = pltpu.make_async_copy(
        k_ref.at[:, pl.ds(pl.multiple_of(z * HD, HD), HD)], kv.at[z + 2, yc, :, 0:HD], loc.at[2]
    )
    own_v = pltpu.make_async_copy(
        v_ref.at[:, pl.ds(pl.multiple_of(z * HD, HD), HD)], kv.at[z + 2, yc, :, HD : 2 * HD], loc.at[3]
    )
    own_w = pltpu.make_async_copy(w_ref, w8.at[yc], loc.at[4])
    own_wk = pltpu.make_async_copy(wk_ref, wkv.at[:, 0], loc.at[5])
    own_wv = pltpu.make_async_copy(wv_ref, wkv.at[:, 1], loc.at[6])
    barrier = pltpu.get_barrier_semaphore()
    for dy in range(2):
        for dz in range(4):
            if dy or dz:
                pl.semaphore_signal(
                    barrier, inc=1, device_id=dev(zoff(dz), lax.rem(y + dy, 2), c), device_id_type=MESH
                )
    pl.semaphore_signal(barrier, inc=1, device_id=core, device_id_type=MESH)

    @pl.when(sec > 0)
    def _():
        pl.semaphore_signal(barrier, inc=1, device_id=(sec - 1, seq), device_id_type=MESH)

    @pl.when(sec < 7)
    def _():
        pl.semaphore_signal(barrier, inc=1, device_id=(sec + 1, seq), device_id_type=MESH)

    for copy in (own_k, own_v, own_q, own_o, own_w, own_wk, own_wv):
        copy.start()
    doc = doc_ref[...]
    first = jnp.zeros_like(doc)
    for value in (1, 2, 3):
        before = jnp.sum((doc < value).astype(F32), axis=1, keepdims=True).astype(jnp.int32)
        first = jnp.where(doc == value, before, first)
    start[...] = first
    kv[0:2] = jnp.zeros((2, 4, ROWS, 2 * HD), BF16)
    dk[...] = jnp.zeros_like(dk)
    dv[...] = jnp.zeros_like(dv)
    own_k.wait()
    own_v.wait()
    with jax.named_scope("barrier"):
        pl.semaphore_wait(barrier, 8 + jnp.where(sec > 0, 1, 0) + jnp.where(sec < 7, 1, 0))

    kv_copies = []
    for d in (1, 3, 2):
        zd = zoff(d)
        cols = pl.ds(pl.multiple_of(zd * HD, HD), HD)
        kv_copies.append(
            (
                remote(k_ref.at[:, cols], kv.at[z + 2, yc, :, 0:HD], kvz_s.at[0, d], kvz_r.at[0, d], dev(zd, y, c)),
                remote(
                    v_ref.at[:, cols], kv.at[z + 2, yc, :, HD : 2 * HD], kvz_s.at[1, d], kvz_r.at[1, d], dev(zd, y, c)
                ),
            )
        )
    for pair in kv_copies:
        pair[0].start()
        pair[1].start()

    def kv_y(d):
        zs = lax.rem(z + 4 - d, 4) + 2
        return remote(kv.at[zs, yc], kv.at[zs, yc], kvy_s.at[d], kvy_r.at[d], ypart)

    def kv_y_in(d):
        zs = lax.rem(z + 4 - d, 4) + 2
        at = (1 - y) * 2 + c
        return remote(kv.at[zs, at], kv.at[zs, at], kvy_s.at[d], kvy_r.at[d], ypart)

    def kv_c(i, d):
        zs = lax.rem(z + 4 - d, 4) + 2
        at = yc if i == 0 else (1 - y) * 2 + c
        return remote(kv.at[zs, at], kv.at[zs, at], kvc_s.at[i, d], kvc_r.at[i, d], core)

    def kv_c_in(i, d):
        zs = lax.rem(z + 4 - d, 4) + 2
        at = (y if i == 0 else 1 - y) * 2 + 1 - c
        return remote(kv.at[zs, at], kv.at[zs, at], kvc_s.at[i, d], kvc_r.at[i, d], core)

    def w_y(n):
        cols = pl.ds(n * CW, CW)
        return remote(w_ref.at[:, cols], w8.at[yc, :, cols], wy_s.at[n], wy_r.at[n], ypart)

    def w_y_in(n):
        cols = pl.ds(n * CW, CW)
        at = (1 - y) * 2 + c
        return remote(w_ref.at[:, cols], w8.at[at, :, cols], wy_s.at[n], wy_r.at[n], ypart)

    w_core = remote(w_ref, w8.at[yc], wc_s.at[0], wc_r.at[0], core)

    def w_fwd(n):
        cols = pl.ds(n * CW, CW)
        at = (1 - y) * 2 + c
        return remote(w8.at[at, :, cols], w8.at[at, :, cols], wf_s.at[n], wf_r.at[n], core)

    def w_fwd_in(n):
        cols = pl.ds(n * CW, CW)
        at = (1 - y) * 2 + 1 - c
        return remote(w8.at[at, :, cols], w8.at[at, :, cols], wf_s.at[n], wf_r.at[n], core)

    qo_copies = {}
    for d in (1, 3, 2):
        zd = zoff(d)
        cols = pl.ds(pl.multiple_of(zd * GW, GW), GW)
        qo_copies[d] = (
            remote(q_ref.at[:, cols], qs.at[z], qo_s.at[0, d], qo_r.at[0, d], dev(zd, y, c)),
            remote(o_ref.at[:, cols], os_.at[z], qo_s.at[1, d], qo_r.at[1, d], dev(zd, y, c)),
        )

    kv_y(0).start()
    kv_c(0, 0).start()
    with jax.named_scope("kvz"):
        for d in (1, 3, 2):
            zs = lax.rem(z + 4 - d, 4)
            remote(k_ref.at[:, 0:HD], kv.at[zs + 2, yc, :, 0:HD], kvz_s.at[0, d], kvz_r.at[0, d], core).wait_recv()
            remote(
                v_ref.at[:, 0:HD], kv.at[zs + 2, yc, :, HD : 2 * HD], kvz_s.at[1, d], kvz_r.at[1, d], core
            ).wait_recv()
            kv_y(d).start()
            kv_c(0, d).start()
    for d in (1, 3, 2):
        for copy in qo_copies[d]:
            copy.start()
    with jax.named_scope("kvy"):
        for d in (0, 1, 3, 2):
            kv_y_in(d).wait_recv()
            kv_c(1, d).start()
    for n in range(W_EARLY):
        w_y(n).start()
    w_core.start()
    with jax.named_scope("kvc"):
        for i in range(2):
            for d in range(4):
                kv_c_in(i, d).wait_recv()

    kv_rows = kv.reshape(24 * ROWS, 2 * HD)

    def attend(i, carry):
        d = jnp.where(i == 2, 3, jnp.where(i == 3, 2, i))
        zb = lax.rem(z + 4 - d, 4)

        with jax.named_scope("qowait"):

            @pl.when(d == 0)
            def _():
                own_q.wait()
                own_o.wait()

            @pl.when(d > 0)
            def _():
                remote(q_ref.at[:, 0:GW], qs.at[zb], qo_s.at[0, d], qo_r.at[0, d], core).wait_recv()
                remote(o_ref.at[:, 0:GW], os_.at[zb], qo_s.at[1, d], qo_r.at[1, d], core).wait_recv()

        block = zb * 4 + yc
        at = pl.multiple_of(block * ROWS, ROWS)
        k_win = kv_rows[pl.ds(at, WIN * ROWS), 0:HD]
        base = (block - 8) * ROWS
        lower = start[:, pl.ds(at, ROWS)] - base
        lower = jnp.concatenate([lower, lower], axis=1)

        def heads(hp, carry):
            cols = pl.ds(pl.multiple_of(hp * 2 * HD, 2 * HD), 2 * HD)
            q2 = qs[zb, :, cols]
            q2 = jnp.concatenate([q2[:, 0:HD], q2[:, HD:]], axis=0)
            o2 = os_[zb, :, cols]
            o2 = jnp.concatenate([o2[:, 0:HD], o2[:, HD:]], axis=0)
            v_win = kv_rows[pl.ds(at, WIN * ROWS), HD : 2 * HD]
            k_win = kv_rows[pl.ds(at, WIN * ROWS), 0:HD]
            nt = (((1,), (1,)), ((), ()))
            s = lax.dot_general(k_win, q2, nt, preferred_element_type=F32)
            key = lax.broadcasted_iota(jnp.int32, (8 * ROWS, 2 * ROWS), 0)
            s_a = jnp.where(key >= lower, s[: 8 * ROWS], NEG)
            key = lax.broadcasted_iota(jnp.int32, (ROWS, 2 * ROWS), 0)
            row = lax.broadcasted_iota(jnp.int32, (ROWS, 2 * ROWS), 1)
            row = jnp.where(row >= ROWS, row - ROWS, row)
            s_b = jnp.where((key + 8 * ROWS >= lower) & (key <= row), s[8 * ROWS :], NEG)
            s = jnp.concatenate([s_a, s_b], axis=0)
            top = jnp.max(s, axis=0, keepdims=True)
            e = jnp.exp2((s - top) * (SCALE * math.log2(math.e)))
            inv = 1.0 / jnp.sum(e, axis=0, keepdims=True)
            dp = lax.dot_general(v_win, o2, nt, preferred_element_type=F32)
            delta = jnp.sum(e * dp, axis=0, keepdims=True) * inv
            p_s[:, cols] = (e * inv).astype(BF16)
            ds_s[:, cols] = (e * (dp - delta) * (inv * SCALE)).astype(BF16)
            return carry

        with jax.named_scope("heads"):
            lax.fori_loop(0, 4, heads, 0)
        with jax.named_scope("grads"):
            qb = qs[zb]
            ob = os_[zb]
            qb = jnp.concatenate([qb[:, h * HD : (h + 1) * HD] for h in range(8)], axis=0)
            ob = jnp.concatenate([ob[:, h * HD : (h + 1) * HD] for h in range(8)], axis=0)
            win = pl.ds(at, WIN * ROWS)
            dv[win, :] += jnp.dot(p_s[...], ob, preferred_element_type=F32)
            dk[win, :] += jnp.dot(ds_s[...], qb, preferred_element_type=F32)
            dqt = lax.dot_general(k_win, ds_s[...], (((0,), (0,)), ((), ())), preferred_element_type=F32)
            for h in range(8):
                dq[pl.ds(pl.multiple_of(zb * ROWS, ROWS), ROWS), h * HD : (h + 1) * HD] = dqt[
                    :, h * HD : (h + 1) * HD
                ].T.astype(BF16)
        return carry

    lax.fori_loop(0, 4, attend, 0)

    def blocks(b, carry):
        rows = pl.ds(pl.multiple_of((b * 2 + 1 - c + 8) * ROWS, ROWS), ROWS)
        at = lax.rem(b, 2)
        dkv_s[at, b // 2, :, 0:HD] = dk[rows, :].astype(BF16)
        dkv_s[at, b // 2, :, HD : 2 * HD] = dv[rows, :].astype(BF16)
        return carry

    lax.fori_loop(0, 8, blocks, 0)
    dkv_core = remote(dkv_s, dkv_c, dc_s.at[0], dc_r.at[0], core)
    dkv_core.start()

    with jax.named_scope("wcore"):
        own_w.wait()
        w_core.wait()

    def dd(dy, dz):
        yy = lax.rem(y + dy, 2)
        zz = zoff(dz)
        return remote(dkv_o.at[yy, zz], dkv_i.at[y, z], dd_s.at[dy, dz], dd_r.at[dy, dz], dev(zz, yy, c))

    up, down = dev(zoff(1), y, c), dev(zoff(3), y, c)

    def half(i, n):
        return remote(half_s.at[i, n], half_r.at[i, n], ra_s.at[i, n], ra_r.at[i, n], up if i == 0 else down)

    def full(i, n):
        return remote(full_s.at[i, n], full_r.at[i, n], rb_s.at[i, n], rb_r.at[i, n], up if i == 0 else down)

    def product(n):
        cols = pl.ds(pl.multiple_of(n * CW, CW), CW)
        slot = lax.rem(n, 2)

        with jax.named_scope("prodwait"):

            @pl.when(n < NC - 1)
            def _():
                w_y_in(n + 1).wait_recv()
                w_fwd(n + 1).start()

            w_fwd_in(n).wait_recv()
        with jax.named_scope("proddot"):
            part[slot] = jnp.dot(dq[...], w8.reshape(GW, D)[:, cols], preferred_element_type=F32)
            own[:, cols] = part[slot, pl.ds(pl.multiple_of(z * ROWS, ROWS), ROWS), :]
            rows = pl.ds(pl.multiple_of(zoff(2) * ROWS, ROWS), ROWS)
            for i in range(2):
                half_s[i, n] = part[slot, rows, i * (CW // 2) : (i + 1) * (CW // 2)].astype(BF16)
            for i in range(2):
                half(i, n).start()

    def merge(n):
        slot = lax.rem(n, 2)
        for i in range(2):
            with jax.named_scope("mergewait"):
                half(i, n).wait_recv()
            rows = pl.ds(pl.multiple_of(zoff(1 if i == 0 else 3) * ROWS, ROWS), ROWS)
            mine = slice(0, CW // 2) if i == 0 else slice(CW // 2, CW)
            rest = slice(CW // 2, CW) if i == 0 else slice(0, CW // 2)
            full_s[i, n, :, mine] = (part[slot, rows, mine] + half_r[i, n].astype(F32)).astype(BF16)
            full_s[i, n, :, rest] = part[slot, rows, rest].astype(BF16)
            full(i, n).start()

    def hop(n):
        cols = pl.ds(n * CW, CW)
        return remote(fin.at[:, cols], out_ref.at[:, cols], hop_s.at[n], hop_r.at[n], (jnp.maximum(sec - 1, 0), seq))

    def finish(n):
        cols = pl.ds(pl.multiple_of(n * CW, CW), CW)
        with jax.named_scope("findot"):
            dkv = jnp.concatenate(
                [(dkv_i[0, zz].astype(F32) + dkv_i[1, zz].astype(F32)).astype(BF16) for zz in range(4)], axis=1
            )
            total = own[:, cols] + jnp.dot(dkv, wkv.reshape(GW, D)[:, cols], preferred_element_type=F32)
        with jax.named_scope("finwait"):
            full(0, n).wait_recv()
            full(1, n).wait_recv()
        total = total + full_r[0, n].astype(F32) + full_r[1, n].astype(F32)
        fin[:, cols] = total.astype(BF16)

        @pl.when(sec > 0)
        def _():
            hop(n).start()

    with jax.named_scope("wy0"):
        w_y_in(0).wait_recv()
    w_fwd(0).start()
    product(0)

    with jax.named_scope("dkvsum"):
        dkv_core.wait_recv()
        for yy in range(2):

            def add(zz, carry):
                rows = pl.ds(pl.multiple_of((zz * 4 + yy * 2 + c + 8) * ROWS, ROWS), ROWS)
                dkv_o[yy, zz, :, 0:HD] = (dk[rows, :] + dkv_c[yy, zz, :, 0:HD].astype(F32)).astype(BF16)
                dkv_o[yy, zz, :, HD : 2 * HD] = (dv[rows, :] + dkv_c[yy, zz, :, HD : 2 * HD].astype(F32)).astype(BF16)
                return carry

            lax.fori_loop(0, 4, add, 0)
    for dy in (1, 0):
        for dz in range(4):
            if dy or dz:
                dd(dy, dz).start()
    dkv_i[y, z] = dkv_o[y, z]
    for n in range(W_EARLY, NC):
        w_y(n).start()
    own_wk.wait()
    own_wv.wait()

    def step(n, carry):
        @pl.when(n < NC)
        def _():
            product(n)

        @pl.when(n <= NC)
        def _():
            merge(n - 1)

        @pl.when(n == LAG)
        def _():
            with jax.named_scope("ddwait"):
                for dy in range(2):
                    for dz in range(4):
                        if dy or dz:
                            ys = lax.rem(y + dy, 2)
                            zs = lax.rem(z + 4 - dz, 4)
                            remote(
                                dkv_o.at[ys, zs], dkv_i.at[ys, zs], dd_s.at[dy, dz], dd_r.at[dy, dz], core
                            ).wait_recv()

        @pl.when(n >= LAG)
        def _():
            finish(n - LAG)

        return carry

    lax.fori_loop(1, NC + LAG, step, 0)

    @pl.when(sec == 7)
    def _():
        out_ref[...] = jnp.zeros_like(out_ref)

    with jax.named_scope("drain"):
        for pair in kv_copies:
            pair[0].wait_send()
            pair[1].wait_send()
        for d in range(4):
            kv_y(d).wait_send()
            kv_c(0, d).wait_send()
            kv_c(1, d).wait_send()
        for d in (1, 2, 3):
            for copy in qo_copies[d]:
                copy.wait_send()
        dkv_core.wait_send()
        for dy in range(2):
            for dz in range(4):
                if dy or dz:
                    dd(dy, dz).wait_send()

        def drain(n, carry):
            w_y(n).wait_send()
            w_fwd(n).wait_send()
            for i in range(2):
                half(i, n).wait_send()
                full(i, n).wait_send()

            @pl.when(sec > 0)
            def _():
                hop(n).wait_send()

            @pl.when(sec < 7)
            def _():
                hop(n).wait_recv()

            return carry

        lax.fori_loop(0, NC, drain, 0)


def body(queries, keys, values, out_grad, documents, query_weight, key_weight, value_weight):
    hbm = pl.BlockSpec(memory_space=pltpu.MemorySpace.HBM)
    vmem = pl.BlockSpec(memory_space=pltpu.VMEM)
    dma = pltpu.SemaphoreType.DMA
    scratch = [
        pltpu.VMEM((4, ROWS, GW), BF16),
        pltpu.VMEM((4, ROWS, GW), BF16),
        pltpu.VMEM((6, 4, ROWS, 2 * HD), BF16),
        pltpu.VMEM((1, 2048), jnp.int32),
        pltpu.VMEM((WIN * ROWS, GW), BF16),
        pltpu.VMEM((WIN * ROWS, GW), BF16),
        pltpu.VMEM((24 * ROWS, HD), F32),
        pltpu.VMEM((24 * ROWS, HD), F32),
        pltpu.VMEM((4 * ROWS, GW), BF16),
        pltpu.VMEM((4, 256, D), BF16),
        pltpu.VMEM((4, 2, HD, D), BF16),
        pltpu.VMEM((2, NC, ROWS, CW // 2), BF16),
        pltpu.VMEM((2, NC, ROWS, CW // 2), BF16),
        pltpu.VMEM((2, NC, ROWS, CW), BF16),
        pltpu.VMEM((2, NC, ROWS, CW), BF16),
        pltpu.VMEM((2, 4 * ROWS, CW), F32),
        pltpu.VMEM((ROWS, D), F32),
        pltpu.VMEM((2, 4, ROWS, 2 * HD), BF16),
        pltpu.VMEM((2, 4, ROWS, 2 * HD), BF16),
        pltpu.VMEM((2, 4, ROWS, 2 * HD), BF16),
        pltpu.VMEM((2, 4, ROWS, 2 * HD), BF16),
        pltpu.VMEM((ROWS, D), BF16),
        dma((7,)),
        dma((2, 4)), dma((2, 4)),
        dma((4,)), dma((4,)),
        dma((2, 4)), dma((2, 4)),
        dma((2, 4)), dma((2, 4)),
        dma((NC,)), dma((NC,)),
        dma((1,)), dma((1,)),
        dma((NC,)), dma((NC,)),
        dma((2, NC)), dma((2, NC)),
        dma((2, NC)), dma((2, NC)),
        dma((1,)), dma((1,)),
        dma((2, 4)), dma((2, 4)),
        dma((NC,)), dma((NC,)),
    ]
    out = pl.pallas_call(
        kernel,
        out_shape=jax.ShapeDtypeStruct((ROWS, D), BF16),
        in_specs=[hbm, hbm, hbm, hbm, vmem, hbm, hbm, hbm],
        out_specs=vmem,
        scratch_shapes=scratch,
        compiler_params=pltpu.CompilerParams(
            collective_id=0, has_side_effects=True, vmem_limit_bytes=67043328
        ),
    )(
        queries[0],
        keys[0],
        values[0],
        out_grad[0],
        documents,
        query_weight[0],
        key_weight[0].reshape(4, HD, D),
        value_weight[0].reshape(4, HD, D),
    )
    return out[None]


def solution(mesh):
    in_specs = (
        P("section", "seq", None),
        P("section", "seq", None),
        P("section", "seq", None),
        P("section", "seq", None),
        P("section", None),
        P("section", "seq", None),
        P("section", None, None),
        P("section", None, None),
    )
    out_specs = P("section", "seq", None)
    return jax.shard_map(body, mesh=mesh, in_specs=in_specs, out_specs=out_specs, check_vma=False)
```

```python
import math

import jax
import jax.numpy as jnp
from jax import lax
from jax.experimental import pallas as pl
from jax.experimental.pallas import tpu as pltpu
from jax.sharding import PartitionSpec as P

HD = 128
ROWS = 128
GW = 1024
D = 4096
NC = 8
CW = D // NC
W_EARLY = 7
EARLY = 3
SLOTS = 8
ORDER = ('w3', 'p0', 'm0', 'core', 'p3', 'p1', 'm1', 'w4', 'p2', 'p4', 'w5', 'p5', 'm2', 'w6', 'p6', 'ysum', 'm3', 'm4', 'm5', 'dkv', 'w7', 'f0', 'f1', 'f2', 'f3', 'p7', 'm6', 'f4', 'f5', 'm7', 'f6', 'f7')
WIN = 9
SCALE = 1.0 / math.sqrt(HD)
NEG = -1e30
MESH = pl.DeviceIdType.MESH
F32 = jnp.float32
BF16 = jnp.bfloat16


def remote(src, dst, send, recv, device):
    return pltpu.make_async_remote_copy(
        src_ref=src, dst_ref=dst, send_sem=send, recv_sem=recv, device_id=device, device_id_type=MESH
    )


def kernel(
    q_ref, k_ref, v_ref, o_ref, doc_ref, w_ref, wk_ref, wv_ref,
    out_ref,
    qs, os_, kv, start, p_s, ds_s, dk, dv, dq, w8, wkv, half_s, half_r, full_s, full_r, part, own,
    dkv_s, dkv_c, dkv_o, dkv_t, dkv_p, dkv_i, fin,
    loc, kvz_s, kvz_r, kvy_s, kvy_r, kvc_s, kvc_r, qo_s, qo_r,
    w0_s, w0_r, wy_s, wy_r, wc_s, wc_r, wf_s, wf_r, ra_s, ra_r, rb_s, rb_r, dc_s, dc_r, dd_s, dd_r, hop_s, hop_r,
):
    sec = lax.axis_index("section")
    seq = lax.axis_index("seq")
    z = seq // 4
    y = lax.rem(seq // 2, 2)
    c = lax.rem(seq, 2)
    yc = y * 2 + c

    def dev(zz, yy, cc):
        return (sec, zz * 4 + yy * 2 + cc)

    def zoff(d):
        return lax.rem(z + d, 4)

    core = dev(z, y, 1 - c)
    ypart = dev(z, 1 - y, c)

    own_q = pltpu.make_async_copy(q_ref.at[:, pl.ds(pl.multiple_of(z * GW, GW), GW)], qs.at[z], loc.at[0])
    own_o = pltpu.make_async_copy(o_ref.at[:, pl.ds(pl.multiple_of(z * GW, GW), GW)], os_.at[z], loc.at[1])
    own_k = pltpu.make_async_copy(
        k_ref.at[:, pl.ds(pl.multiple_of(z * HD, HD), HD)], kv.at[z + 2, yc, :, 0:HD], loc.at[2]
    )
    own_v = pltpu.make_async_copy(
        v_ref.at[:, pl.ds(pl.multiple_of(z * HD, HD), HD)], kv.at[z + 2, yc, :, HD : 2 * HD], loc.at[3]
    )
    own_w = pltpu.make_async_copy(w_ref, w8.at[yc], loc.at[4])
    own_wk = pltpu.make_async_copy(wk_ref, wkv.at[:, 0], loc.at[5])
    own_wv = pltpu.make_async_copy(wv_ref, wkv.at[:, 1], loc.at[6])
    barrier = pltpu.get_barrier_semaphore()
    for partner in (dev(zoff(1), y, c), dev(zoff(2), y, c), dev(zoff(3), y, c), ypart, core):
        pl.semaphore_signal(barrier, inc=1, device_id=partner, device_id_type=MESH)

    @pl.when(sec > 0)
    def _():
        pl.semaphore_signal(barrier, inc=1, device_id=(sec - 1, seq), device_id_type=MESH)

    @pl.when(sec < 7)
    def _():
        pl.semaphore_signal(barrier, inc=1, device_id=(sec + 1, seq), device_id_type=MESH)

    for copy in (own_k, own_v, own_q, own_o, own_w, own_wk, own_wv):
        copy.start()
    doc = doc_ref[...]
    first = jnp.zeros_like(doc)
    for value in (1, 2, 3):
        before = jnp.sum((doc < value).astype(F32), axis=1, keepdims=True).astype(jnp.int32)
        first = jnp.where(doc == value, before, first)
    start[...] = first
    kv[0:2] = jnp.zeros((2, 4, ROWS, 2 * HD), BF16)
    dk[...] = jnp.zeros_like(dk)
    dv[...] = jnp.zeros_like(dv)
    own_k.wait()
    own_v.wait()
    with jax.named_scope("barrier"):
        pl.semaphore_wait(barrier, 5 + jnp.where(sec > 0, 1, 0) + jnp.where(sec < 7, 1, 0))

    kv_copies = []
    for d in (1, 3, 2):
        zd = zoff(d)
        cols = pl.ds(pl.multiple_of(zd * HD, HD), HD)
        kv_copies.append(
            (
                remote(k_ref.at[:, cols], kv.at[z + 2, yc, :, 0:HD], kvz_s.at[0, d], kvz_r.at[0, d], dev(zd, y, c)),
                remote(
                    v_ref.at[:, cols], kv.at[z + 2, yc, :, HD : 2 * HD], kvz_s.at[1, d], kvz_r.at[1, d], dev(zd, y, c)
                ),
            )
        )
    for pair in kv_copies:
        pair[0].start()
        pair[1].start()

    def kv_y(d):
        zs = lax.rem(z + 4 - d, 4) + 2
        return remote(kv.at[zs, yc], kv.at[zs, yc], kvy_s.at[d], kvy_r.at[d], ypart)

    def kv_y_in(d):
        zs = lax.rem(z + 4 - d, 4) + 2
        at = (1 - y) * 2 + c
        return remote(kv.at[zs, at], kv.at[zs, at], kvy_s.at[d], kvy_r.at[d], ypart)

    def kv_c(i, d):
        zs = lax.rem(z + 4 - d, 4) + 2
        at = yc if i == 0 else (1 - y) * 2 + c
        return remote(kv.at[zs, at], kv.at[zs, at], kvc_s.at[i, d], kvc_r.at[i, d], core)

    def kv_c_in(i, d):
        zs = lax.rem(z + 4 - d, 4) + 2
        at = (y if i == 0 else 1 - y) * 2 + 1 - c
        return remote(kv.at[zs, at], kv.at[zs, at], kvc_s.at[i, d], kvc_r.at[i, d], core)

    def w_y0(i):
        cols = pl.ds(i * (CW // 2), CW // 2)
        return remote(w_ref.at[:, cols], w8.at[yc, :, cols], w0_s.at[i], w0_r.at[i], ypart)

    def w_y0_in(i):
        cols = pl.ds(i * (CW // 2), CW // 2)
        at = (1 - y) * 2 + c
        return remote(w_ref.at[:, cols], w8.at[at, :, cols], w0_s.at[i], w0_r.at[i], ypart)

    def w_y(n):
        cols = pl.ds(n * CW, CW)
        return remote(w_ref.at[:, cols], w8.at[yc, :, cols], wy_s.at[n], wy_r.at[n], ypart)

    def w_y_in(n):
        cols = pl.ds(n * CW, CW)
        at = (1 - y) * 2 + c
        return remote(w_ref.at[:, cols], w8.at[at, :, cols], wy_s.at[n], wy_r.at[n], ypart)

    w_core = remote(w_ref, w8.at[yc], wc_s.at[0], wc_r.at[0], core)

    def w_fwd(n):
        cols = pl.ds(n * CW, CW)
        at = (1 - y) * 2 + c
        return remote(w8.at[at, :, cols], w8.at[at, :, cols], wf_s.at[n], wf_r.at[n], core)

    def w_fwd_in(n):
        cols = pl.ds(n * CW, CW)
        at = (1 - y) * 2 + 1 - c
        return remote(w8.at[at, :, cols], w8.at[at, :, cols], wf_s.at[n], wf_r.at[n], core)

    qo_copies = {}
    for d in (1, 3, 2):
        zd = zoff(d)
        cols = pl.ds(pl.multiple_of(zd * GW, GW), GW)
        qo_copies[d] = (
            remote(q_ref.at[:, cols], qs.at[z], qo_s.at[0, d], qo_r.at[0, d], dev(zd, y, c)),
            remote(o_ref.at[:, cols], os_.at[z], qo_s.at[1, d], qo_r.at[1, d], dev(zd, y, c)),
        )

    kv_y(0).start()
    kv_c(0, 0).start()
    w_y0(0).start()
    with jax.named_scope("kvz"):
        for d in (1, 3, 2):
            zs = lax.rem(z + 4 - d, 4)
            remote(k_ref.at[:, 0:HD], kv.at[zs + 2, yc, :, 0:HD], kvz_s.at[0, d], kvz_r.at[0, d], core).wait_recv()
            remote(
                v_ref.at[:, 0:HD], kv.at[zs + 2, yc, :, HD : 2 * HD], kvz_s.at[1, d], kvz_r.at[1, d], core
            ).wait_recv()
            kv_y(d).start()
            kv_c(0, d).start()
    for d in (1, 3, 2):
        for copy in qo_copies[d]:
            copy.start()
    w_y0(1).start()
    for n in range(1, W_EARLY):
        w_y(n).start()
    with jax.named_scope("kvy"):
        for d in (0, 1, 3, 2):
            kv_y_in(d).wait_recv()
            kv_c(1, d).start()
    w_core.start()
    with jax.named_scope("kvc"):
        for i in range(2):
            for d in range(4):
                kv_c_in(i, d).wait_recv()

    kv_rows = kv.reshape(24 * ROWS, 2 * HD)
    w_rows = w8.reshape(GW, D)
    up, down = dev(zoff(1), y, c), dev(zoff(3), y, c)
    far = pl.ds(pl.multiple_of(zoff(2) * ROWS, ROWS), ROWS)

    def half(i, n):
        return remote(half_s.at[i, n], half_r.at[i, n], ra_s.at[i, n], ra_r.at[i, n], up if i == 0 else down)

    def full(i, n):
        return remote(full_s.at[i, n], full_r.at[i, n], rb_s.at[i, n], rb_r.at[i, n], up if i == 0 else down)

    def forward(n, carry):
        w_y_in(n).wait_recv()
        w_fwd(n).start()
        return carry

    def forward_early(n, carry):
        @pl.when(n == 0)
        def _():
            w_y0_in(0).wait_recv()
            w_y0_in(1).wait_recv()

        @pl.when(n > 0)
        def _():
            w_y_in(n).wait_recv()

        w_fwd(n).start()
        return carry

    def early(n, carry):
        cols = pl.ds(pl.multiple_of(n * CW, CW), CW)
        w_fwd_in(n).wait_recv()
        res = jnp.dot(dq[far, :], w_rows[:, cols], preferred_element_type=F32).astype(BF16)
        for i in range(2):
            half_s[i, n] = res[:, i * (CW // 2) : (i + 1) * (CW // 2)]
            half(i, n).start()
        return carry

    def attend(i, carry):
        d = jnp.where(i == 2, 3, jnp.where(i == 3, 2, i))
        zb = lax.rem(z + 4 - d, 4)
        lo, hi = jnp.where(i == 3, 0, 0), jnp.where(i == 3, 3, 0)

        with jax.named_scope("qowait"):

            @pl.when(d == 0)
            def _():
                own_q.wait()
                own_o.wait()

            @pl.when(d > 0)
            def _():
                remote(q_ref.at[:, 0:GW], qs.at[zb], qo_s.at[0, d], qo_r.at[0, d], core).wait_recv()
                remote(o_ref.at[:, 0:GW], os_.at[zb], qo_s.at[1, d], qo_r.at[1, d], core).wait_recv()

        @pl.when(i == 1)
        def _():
            own_w.wait()
            w_core.wait()

        with jax.named_scope("forward"):
            lax.fori_loop(lo, hi, forward_early, 0)
        block = zb * 4 + yc
        at = pl.multiple_of(block * ROWS, ROWS)
        k_win = kv_rows[pl.ds(at, WIN * ROWS), 0:HD]
        base = (block - 8) * ROWS
        lower = start[:, pl.ds(at, ROWS)] - base
        lower = jnp.concatenate([lower, lower], axis=1)

        def heads(hp, carry):
            cols = pl.ds(pl.multiple_of(hp * 2 * HD, 2 * HD), 2 * HD)
            q2 = qs[zb, :, cols]
            q2 = jnp.concatenate([q2[:, 0:HD], q2[:, HD:]], axis=0)
            o2 = os_[zb, :, cols]
            o2 = jnp.concatenate([o2[:, 0:HD], o2[:, HD:]], axis=0)
            v_win = kv_rows[pl.ds(at, WIN * ROWS), HD : 2 * HD]
            k_win = kv_rows[pl.ds(at, WIN * ROWS), 0:HD]
            nt = (((1,), (1,)), ((), ()))
            s = lax.dot_general(k_win, q2, nt, preferred_element_type=F32)
            key = lax.broadcasted_iota(jnp.int32, (8 * ROWS, 2 * ROWS), 0)
            s_a = jnp.where(key >= lower, s[: 8 * ROWS], NEG)
            key = lax.broadcasted_iota(jnp.int32, (ROWS, 2 * ROWS), 0)
            row = lax.broadcasted_iota(jnp.int32, (ROWS, 2 * ROWS), 1)
            row = jnp.where(row >= ROWS, row - ROWS, row)
            s_b = jnp.where((key + 8 * ROWS >= lower) & (key <= row), s[8 * ROWS :], NEG)
            s = jnp.concatenate([s_a, s_b], axis=0)
            top = jnp.max(s, axis=0, keepdims=True)
            e = jnp.exp2((s - top) * (SCALE * math.log2(math.e)))
            inv = 1.0 / jnp.sum(e, axis=0, keepdims=True)
            dp = lax.dot_general(v_win, o2, nt, preferred_element_type=F32)
            delta = jnp.sum(e * dp, axis=0, keepdims=True) * inv
            p_s[:, cols] = (e * inv).astype(BF16)
            ds_s[:, cols] = (e * (dp - delta) * (inv * SCALE)).astype(BF16)
            return carry

        with jax.named_scope("heads"):
            lax.fori_loop(0, 4, heads, 0, unroll=4)
        with jax.named_scope("grads"):
            qb = qs[zb]
            ob = os_[zb]
            qb = jnp.concatenate([qb[:, h * HD : (h + 1) * HD] for h in range(8)], axis=0)
            ob = jnp.concatenate([ob[:, h * HD : (h + 1) * HD] for h in range(8)], axis=0)
            win = pl.ds(at, WIN * ROWS)
            dv[win, :] += jnp.dot(p_s[...], ob, preferred_element_type=F32)
            dk[win, :] += jnp.dot(ds_s[...], qb, preferred_element_type=F32)
            dqt = lax.dot_general(k_win, ds_s[...], (((0,), (0,)), ((), ())), preferred_element_type=F32)
            for h in range(8):
                dq[pl.ds(pl.multiple_of(zb * ROWS, ROWS), ROWS), h * HD : (h + 1) * HD] = dqt[
                    :, h * HD : (h + 1) * HD
                ].T.astype(BF16)
        with jax.named_scope("early"):
            lax.fori_loop(lo, hi, early, 0)
        return carry

    lax.fori_loop(0, 4, attend, 0)

    def blocks(b, carry):
        rows = pl.ds(pl.multiple_of((b * 2 + 1 - c + 8) * ROWS, ROWS), ROWS)
        at = lax.rem(b, 2)
        dkv_s[at, b // 2, :, 0:HD] = dk[rows, :].astype(BF16)
        dkv_s[at, b // 2, :, HD : 2 * HD] = dv[rows, :].astype(BF16)
        return carry

    lax.fori_loop(0, 8, blocks, 0)
    dkv_core = remote(dkv_s, dkv_c, dc_s.at[0], dc_r.at[0], core)
    dkv_core.start()

    def dd_y(i):
        return remote(dkv_o.at[1 - y], dkv_t, dd_s.at[0], dd_r.at[0], ypart)

    def dd_z(d):
        zz = zoff(d)
        return remote(dkv_p.at[zz], dkv_i.at[z], dd_s.at[d], dd_r.at[d], dev(zz, y, c))

    def product(n):
        cols = slice(n * CW, (n + 1) * CW)
        slot = n % SLOTS
        if n >= EARLY:
            with jax.named_scope("prodwait"):
                w_fwd_in(n).wait_recv()
        with jax.named_scope("proddot"):
            part[slot] = jnp.dot(dq[...], w_rows[:, cols], preferred_element_type=F32)
            own[:, cols] = part[slot, pl.ds(pl.multiple_of(z * ROWS, ROWS), ROWS), :]
            if n >= EARLY:
                for i in range(2):
                    half_s[i, n] = part[slot, far, i * (CW // 2) : (i + 1) * (CW // 2)].astype(BF16)
                for i in range(2):
                    half(i, n).start()

    def merge(n):
        slot = n % SLOTS
        for i in range(2):
            with jax.named_scope("mergewait"):
                half(i, n).wait_recv()
            rows = pl.ds(pl.multiple_of(zoff(1 if i == 0 else 3) * ROWS, ROWS), ROWS)
            mine = slice(0, CW // 2) if i == 0 else slice(CW // 2, CW)
            rest = slice(CW // 2, CW) if i == 0 else slice(0, CW // 2)
            full_s[i, n, :, mine] = (part[slot, rows, mine] + half_r[i, n].astype(F32)).astype(BF16)
            full_s[i, n, :, rest] = part[slot, rows, rest].astype(BF16)
            full(i, n).start()

    def hop(n):
        cols = pl.ds(n * CW, CW)
        return remote(fin.at[:, cols], out_ref.at[:, cols], hop_s.at[n], hop_r.at[n], (jnp.maximum(sec - 1, 0), seq))

    def finish(n):
        cols = slice(n * CW, (n + 1) * CW)
        with jax.named_scope("findot"):
            dkv = jnp.concatenate([dkv_i[zz] for zz in range(4)], axis=1)
            total = own[:, cols] + jnp.dot(dkv, wkv.reshape(GW, D)[:, cols], preferred_element_type=F32)
        with jax.named_scope("finwait"):
            full(0, n).wait_recv()
            full(1, n).wait_recv()
        total = total + full_r[0, n].astype(F32) + full_r[1, n].astype(F32)
        fin[:, cols] = total.astype(BF16)

        @pl.when(sec > 0)
        def _():
            hop(n).start()

    def dkv_core_sum():
        dkv_core.wait_recv()
        for yy in range(2):

            def add(zz, carry):
                rows = pl.ds(pl.multiple_of((zz * 4 + yy * 2 + c + 8) * ROWS, ROWS), ROWS)
                dkv_o[yy, zz, :, 0:HD] = (dk[rows, :] + dkv_c[yy, zz, :, 0:HD].astype(F32)).astype(BF16)
                dkv_o[yy, zz, :, HD : 2 * HD] = (dv[rows, :] + dkv_c[yy, zz, :, HD : 2 * HD].astype(F32)).astype(BF16)
                return carry

            lax.fori_loop(0, 4, add, 0)
        dd_y(0).start()
        for n in range(W_EARLY, NC):
            w_y(n).start()

    def dkv_y_sum():
        dd_y(0).wait_recv()

        def add(zz, carry):
            dkv_p[zz] = (dkv_o[y, zz].astype(F32) + dkv_t[zz].astype(F32)).astype(BF16)
            return carry

        lax.fori_loop(0, 4, add, 0)
        for d in (2, 1, 3):
            dd_z(d).start()
        dkv_i[z] = dkv_p[z]
        own_wk.wait()
        own_wv.wait()

    def dkv_arrived():
        for d in (2, 1, 3):
            zs = lax.rem(z + 4 - d, 4)
            remote(dkv_p.at[zs], dkv_i.at[zs], dd_s.at[d], dd_r.at[d], core).wait_recv()

    steps = {"p": product, "m": merge, "f": finish, "w": lambda n: forward(n, 0)}
    for step in ORDER:
        if step == "core":
            with jax.named_scope("dkvcore"):
                dkv_core_sum()
        elif step == "ysum":
            with jax.named_scope("ddywait"):
                dkv_y_sum()
        elif step == "dkv":
            with jax.named_scope("ddwait"):
                dkv_arrived()
        else:
            with jax.named_scope(step):
                steps[step[0]](int(step[1:]))

    @pl.when(sec == 7)
    def _():
        out_ref[...] = jnp.zeros_like(out_ref)

    with jax.named_scope("drain"):
        for pair in kv_copies:
            pair[0].wait_send()
            pair[1].wait_send()
        for d in range(4):
            kv_y(d).wait_send()
            kv_c(0, d).wait_send()
            kv_c(1, d).wait_send()
        for d in (1, 2, 3):
            for copy in qo_copies[d]:
                copy.wait_send()
        dkv_core.wait_send()
        dd_y(0).wait_send()
        for d in (1, 2, 3):
            dd_z(d).wait_send()

        def drain(n, carry):
            @pl.when(n > 0)
            def _():
                w_y(n).wait_send()

            w_fwd(n).wait_send()
            for i in range(2):
                half(i, n).wait_send()
                full(i, n).wait_send()

            @pl.when(sec > 0)
            def _():
                hop(n).wait_send()

            @pl.when(sec < 7)
            def _():
                hop(n).wait_recv()

            return carry

        w_y0(0).wait_send()
        w_y0(1).wait_send()
        lax.fori_loop(0, NC, drain, 0)


def body(queries, keys, values, out_grad, documents, query_weight, key_weight, value_weight):
    hbm = pl.BlockSpec(memory_space=pltpu.MemorySpace.HBM)
    vmem = pl.BlockSpec(memory_space=pltpu.VMEM)
    dma = pltpu.SemaphoreType.DMA
    scratch = [
        pltpu.VMEM((4, ROWS, GW), BF16),
        pltpu.VMEM((4, ROWS, GW), BF16),
        pltpu.VMEM((6, 4, ROWS, 2 * HD), BF16),
        pltpu.VMEM((1, 2048), jnp.int32),
        pltpu.VMEM((WIN * ROWS, GW), BF16),
        pltpu.VMEM((WIN * ROWS, GW), BF16),
        pltpu.VMEM((24 * ROWS, HD), F32),
        pltpu.VMEM((24 * ROWS, HD), F32),
        pltpu.VMEM((4 * ROWS, GW), BF16),
        pltpu.VMEM((4, 256, D), BF16),
        pltpu.VMEM((4, 2, HD, D), BF16),
        pltpu.VMEM((2, NC, ROWS, CW // 2), BF16),
        pltpu.VMEM((2, NC, ROWS, CW // 2), BF16),
        pltpu.VMEM((2, NC, ROWS, CW), BF16),
        pltpu.VMEM((2, NC, ROWS, CW), BF16),
        pltpu.VMEM((SLOTS, 4 * ROWS, CW), F32),
        pltpu.VMEM((ROWS, D), F32),
        pltpu.VMEM((2, 4, ROWS, 2 * HD), BF16),
        pltpu.VMEM((2, 4, ROWS, 2 * HD), BF16),
        pltpu.VMEM((2, 4, ROWS, 2 * HD), BF16),
        pltpu.VMEM((4, ROWS, 2 * HD), BF16),
        pltpu.VMEM((4, ROWS, 2 * HD), BF16),
        pltpu.VMEM((4, ROWS, 2 * HD), BF16),
        pltpu.VMEM((ROWS, D), BF16),
        dma((7,)),
        dma((2, 4)), dma((2, 4)),
        dma((4,)), dma((4,)),
        dma((2, 4)), dma((2, 4)),
        dma((2, 4)), dma((2, 4)),
        dma((2,)), dma((2,)),
        dma((NC,)), dma((NC,)),
        dma((1,)), dma((1,)),
        dma((NC,)), dma((NC,)),
        dma((2, NC)), dma((2, NC)),
        dma((2, NC)), dma((2, NC)),
        dma((1,)), dma((1,)),
        dma((4,)), dma((4,)),
        dma((NC,)), dma((NC,)),
    ]
    out = pl.pallas_call(
        kernel,
        out_shape=pltpu.VMEM((ROWS, D), BF16),
        in_specs=[hbm, hbm, hbm, hbm, vmem, hbm, hbm, hbm],
        out_specs=vmem,
        scratch_shapes=scratch,
        compiler_params=pltpu.CompilerParams(
            collective_id=0, has_side_effects=True, vmem_limit_bytes=60817408
        ),
    )(
        queries[0],
        keys[0],
        values[0],
        out_grad[0],
        documents,
        query_weight[0],
        key_weight[0].reshape(4, HD, D),
        value_weight[0].reshape(4, HD, D),
    )
    return out[None]


def solution(mesh):
    in_specs = (
        P("section", "seq", None),
        P("section", "seq", None),
        P("section", "seq", None),
        P("section", "seq", None),
        P("section", None),
        P("section", "seq", None),
        P("section", None, None),
        P("section", None, None),
    )
    out_specs = P("section", "seq", None)
    return jax.shard_map(body, mesh=mesh, in_specs=in_specs, out_specs=out_specs, check_vma=False)
```

```python
import math

import jax
import jax.numpy as jnp
from jax import lax
from jax.experimental import pallas as pl
from jax.experimental.pallas import tpu as pltpu
from jax.sharding import PartitionSpec as P

HD = 128
ROWS = 128
GW = 1024
D = 4096
NC = 8
CW = D // NC
W_EARLY = 7
EARLY = 3
SLOTS = 6
ORDER = (
    "w3", "core", "p0", "m0", "p3", "p1", "m1", "w4", "p2", "p4", "w5", "p5", "m2", "w6", "p6", "ysum", "m3",
    "m4", "dkv", "f0", "f1", "m5", "w7", "f2", "f3", "p7", "m6", "f4", "f5", "m7", "f6", "f7",
)
WIN = 9
SCALE = 1.0 / math.sqrt(HD)
NEG = -1e30
MESH = pl.DeviceIdType.MESH
F32 = jnp.float32
BF16 = jnp.bfloat16


def remote(src, dst, send, recv, device):
    return pltpu.make_async_remote_copy(
        src_ref=src, dst_ref=dst, send_sem=send, recv_sem=recv, device_id=device, device_id_type=MESH
    )


def kernel(
    q_ref, k_ref, v_ref, o_ref, doc_ref, w_ref, wk_ref, wv_ref,
    out_ref,
    qs, os_, kv, start, p_s, ds_s, dk, dv, dq, w8, wkv, half_s, half_r, full_s, full_r, part, own,
    dkv_s, dkv_c, dkv_o, dkv_t, dkv_p, dkv_i, fin,
    loc, kvz_s, kvz_r, kvy_s, kvy_r, kvc_s, kvc_r, qo_s, qo_r,
    w0_s, w0_r, wy_s, wy_r, wc_s, wc_r, wf_s, wf_r, ra_s, ra_r, rb_s, rb_r, dc_s, dc_r, dd_s, dd_r, hop_s, hop_r,
):
    sec = lax.axis_index("section")
    seq = lax.axis_index("seq")
    z = seq // 4
    y = lax.rem(seq // 2, 2)
    c = lax.rem(seq, 2)
    yc = y * 2 + c

    def dev(zz, yy, cc):
        return (sec, zz * 4 + yy * 2 + cc)

    def zoff(d):
        return lax.rem(z + d, 4)

    core = dev(z, y, 1 - c)
    ypart = dev(z, 1 - y, c)

    own_q = pltpu.make_async_copy(q_ref.at[:, pl.ds(pl.multiple_of(z * GW, GW), GW)], qs.at[z], loc.at[0])
    own_o = pltpu.make_async_copy(o_ref.at[:, pl.ds(pl.multiple_of(z * GW, GW), GW)], os_.at[z], loc.at[1])
    own_k = pltpu.make_async_copy(
        k_ref.at[:, pl.ds(pl.multiple_of(z * HD, HD), HD)], kv.at[z + 2, yc, :, 0:HD], loc.at[2]
    )
    own_v = pltpu.make_async_copy(
        v_ref.at[:, pl.ds(pl.multiple_of(z * HD, HD), HD)], kv.at[z + 2, yc, :, HD : 2 * HD], loc.at[3]
    )
    own_w = pltpu.make_async_copy(w_ref, w8.at[yc], loc.at[4])
    own_wk = pltpu.make_async_copy(wk_ref, wkv.at[:, 0], loc.at[5])
    own_wv = pltpu.make_async_copy(wv_ref, wkv.at[:, 1], loc.at[6])
    barrier = pltpu.get_barrier_semaphore()
    for partner in (dev(zoff(1), y, c), dev(zoff(2), y, c), dev(zoff(3), y, c), ypart, core):
        pl.semaphore_signal(barrier, inc=1, device_id=partner, device_id_type=MESH)

    @pl.when(sec > 0)
    def _():
        pl.semaphore_signal(barrier, inc=1, device_id=(sec - 1, seq), device_id_type=MESH)

    @pl.when(sec < 7)
    def _():
        pl.semaphore_signal(barrier, inc=1, device_id=(sec + 1, seq), device_id_type=MESH)

    for copy in (own_k, own_v, own_q, own_o, own_w, own_wk, own_wv):
        copy.start()
    doc = doc_ref[...]
    first = jnp.zeros_like(doc)
    for value in (1, 2, 3):
        before = jnp.sum((doc < value).astype(F32), axis=1, keepdims=True).astype(jnp.int32)
        first = jnp.where(doc == value, before, first)
    start[...] = first
    kv[0:2] = jnp.zeros((2, 4, ROWS, 2 * HD), BF16)
    dk[...] = jnp.zeros_like(dk)
    dv[...] = jnp.zeros_like(dv)
    own_k.wait()
    own_v.wait()
    with jax.named_scope("barrier"):
        pl.semaphore_wait(barrier, 5 + jnp.where(sec > 0, 1, 0) + jnp.where(sec < 7, 1, 0))

    kv_copies = []
    for d in (1, 3, 2):
        zd = zoff(d)
        cols = pl.ds(pl.multiple_of(zd * HD, HD), HD)
        kv_copies.append(
            (
                remote(k_ref.at[:, cols], kv.at[z + 2, yc, :, 0:HD], kvz_s.at[0, d], kvz_r.at[0, d], dev(zd, y, c)),
                remote(
                    v_ref.at[:, cols], kv.at[z + 2, yc, :, HD : 2 * HD], kvz_s.at[1, d], kvz_r.at[1, d], dev(zd, y, c)
                ),
            )
        )
    for pair in kv_copies:
        pair[0].start()
        pair[1].start()

    def kv_y(d):
        zs = lax.rem(z + 4 - d, 4) + 2
        return remote(kv.at[zs, yc], kv.at[zs, yc], kvy_s.at[d], kvy_r.at[d], ypart)

    def kv_y_in(d):
        zs = lax.rem(z + 4 - d, 4) + 2
        at = (1 - y) * 2 + c
        return remote(kv.at[zs, at], kv.at[zs, at], kvy_s.at[d], kvy_r.at[d], ypart)

    def kv_c(i, d):
        zs = lax.rem(z + 4 - d, 4) + 2
        at = yc if i == 0 else (1 - y) * 2 + c
        return remote(kv.at[zs, at], kv.at[zs, at], kvc_s.at[i, d], kvc_r.at[i, d], core)

    def kv_c_in(i, d):
        zs = lax.rem(z + 4 - d, 4) + 2
        at = (y if i == 0 else 1 - y) * 2 + 1 - c
        return remote(kv.at[zs, at], kv.at[zs, at], kvc_s.at[i, d], kvc_r.at[i, d], core)

    def w_y0(i):
        cols = pl.ds(i * (CW // 2), CW // 2)
        return remote(w_ref.at[:, cols], w8.at[yc, :, cols], w0_s.at[i], w0_r.at[i], ypart)

    def w_y0_in(i):
        cols = pl.ds(i * (CW // 2), CW // 2)
        at = (1 - y) * 2 + c
        return remote(w_ref.at[:, cols], w8.at[at, :, cols], w0_s.at[i], w0_r.at[i], ypart)

    def w_y(n):
        cols = pl.ds(n * CW, CW)
        return remote(w_ref.at[:, cols], w8.at[yc, :, cols], wy_s.at[n], wy_r.at[n], ypart)

    def w_y_in(n):
        cols = pl.ds(n * CW, CW)
        at = (1 - y) * 2 + c
        return remote(w_ref.at[:, cols], w8.at[at, :, cols], wy_s.at[n], wy_r.at[n], ypart)

    w_core = remote(w_ref, w8.at[yc], wc_s.at[0], wc_r.at[0], core)

    def w_fwd(n):
        cols = pl.ds(n * CW, CW)
        at = (1 - y) * 2 + c
        return remote(w8.at[at, :, cols], w8.at[at, :, cols], wf_s.at[n], wf_r.at[n], core)

    def w_fwd_in(n):
        cols = pl.ds(n * CW, CW)
        at = (1 - y) * 2 + 1 - c
        return remote(w8.at[at, :, cols], w8.at[at, :, cols], wf_s.at[n], wf_r.at[n], core)

    qo_copies = {}
    for d in (1, 3, 2):
        zd = zoff(d)
        cols = pl.ds(pl.multiple_of(zd * GW, GW), GW)
        qo_copies[d] = (
            remote(q_ref.at[:, cols], qs.at[z], qo_s.at[0, d], qo_r.at[0, d], dev(zd, y, c)),
            remote(o_ref.at[:, cols], os_.at[z], qo_s.at[1, d], qo_r.at[1, d], dev(zd, y, c)),
        )

    kv_y(0).start()
    kv_c(0, 0).start()
    w_y0(0).start()
    with jax.named_scope("kvz"):
        for d in (1, 3, 2):
            zs = lax.rem(z + 4 - d, 4)
            remote(k_ref.at[:, 0:HD], kv.at[zs + 2, yc, :, 0:HD], kvz_s.at[0, d], kvz_r.at[0, d], core).wait_recv()
            remote(
                v_ref.at[:, 0:HD], kv.at[zs + 2, yc, :, HD : 2 * HD], kvz_s.at[1, d], kvz_r.at[1, d], core
            ).wait_recv()
            kv_y(d).start()
            kv_c(0, d).start()
    for d in (1, 3, 2):
        for copy in qo_copies[d]:
            copy.start()
    w_y0(1).start()
    for n in range(1, W_EARLY):
        w_y(n).start()
    with jax.named_scope("kvy"):
        for d in (0, 1, 3, 2):
            kv_y_in(d).wait_recv()
            kv_c(1, d).start()
    w_core.start()
    with jax.named_scope("kvc"):
        for i in range(2):
            for d in range(4):
                kv_c_in(i, d).wait_recv()

    kv_rows = kv.reshape(24 * ROWS, 2 * HD)
    w_rows = w8.reshape(GW, D)
    up, down = dev(zoff(1), y, c), dev(zoff(3), y, c)
    far = pl.ds(pl.multiple_of(zoff(2) * ROWS, ROWS), ROWS)

    def half(i, n):
        return remote(half_s.at[i, n], half_r.at[i, n], ra_s.at[i, n], ra_r.at[i, n], up if i == 0 else down)

    def full(i, n):
        return remote(full_s.at[i, n], full_r.at[i, n], rb_s.at[i, n], rb_r.at[i, n], up if i == 0 else down)

    def forward(n, carry):
        w_y_in(n).wait_recv()
        w_fwd(n).start()
        return carry

    def forward_early(n, carry):
        @pl.when(n == 0)
        def _():
            w_y0_in(0).wait_recv()
            w_y0_in(1).wait_recv()

        @pl.when(n > 0)
        def _():
            w_y_in(n).wait_recv()

        w_fwd(n).start()
        return carry

    def early(n, carry):
        cols = pl.ds(pl.multiple_of(n * CW, CW), CW)
        w_fwd_in(n).wait_recv()
        res = jnp.dot(dq[far, :], w_rows[:, cols], preferred_element_type=F32).astype(BF16)
        for i in range(2):
            half_s[i, n] = res[:, i * (CW // 2) : (i + 1) * (CW // 2)]
            half(i, n).start()
        return carry

    def attend_block(zb, at, key_at, win):
        keys = win * ROWS
        base = at - 8 * ROWS if win == WIN else 0
        lower = start[:, pl.ds(at, ROWS)] - base
        lower = jnp.concatenate([lower, lower], axis=1)
        kv_win = pl.ds(key_at, keys)

        def heads(hp, carry):
            cols = pl.ds(pl.multiple_of(hp * 2 * HD, 2 * HD), 2 * HD)
            q2 = qs[zb, :, cols]
            q2 = jnp.concatenate([q2[:, 0:HD], q2[:, HD:]], axis=0)
            o2 = os_[zb, :, cols]
            o2 = jnp.concatenate([o2[:, 0:HD], o2[:, HD:]], axis=0)
            v_win = kv_rows[kv_win, HD : 2 * HD]
            k_win = kv_rows[kv_win, 0:HD]
            nt = (((1,), (1,)), ((), ()))
            s = lax.dot_general(k_win, q2, nt, preferred_element_type=F32)
            free = 8 * ROWS if win == WIN else 0
            rest = keys - free
            key = lax.broadcasted_iota(jnp.int32, (rest, 2 * ROWS), 0) + free
            row = lax.broadcasted_iota(jnp.int32, (rest, 2 * ROWS), 1)
            row = jnp.where(row >= ROWS, row - ROWS, row) + (free if win == WIN else yc * ROWS)
            s_b = jnp.where((key >= lower) & (key <= row), s[free:], NEG)
            if free:
                key = lax.broadcasted_iota(jnp.int32, (free, 2 * ROWS), 0)
                s_b = jnp.concatenate([jnp.where(key >= lower, s[:free], NEG), s_b], axis=0)
            s = s_b
            top = jnp.max(s, axis=0, keepdims=True)
            e = jnp.exp2((s - top) * (SCALE * math.log2(math.e)))
            inv = 1.0 / jnp.sum(e, axis=0, keepdims=True)
            dp = lax.dot_general(v_win, o2, nt, preferred_element_type=F32)
            delta = jnp.sum(e * dp, axis=0, keepdims=True) * inv
            p_s[0:keys, cols] = (e * inv).astype(BF16)
            ds_s[0:keys, cols] = (e * (dp - delta) * (inv * SCALE)).astype(BF16)
            return carry

        with jax.named_scope("heads"):
            lax.fori_loop(0, 4, heads, 0, unroll=4)
        with jax.named_scope("grads"):
            qb = qs[zb]
            ob = os_[zb]
            qb = jnp.concatenate([qb[:, h * HD : (h + 1) * HD] for h in range(8)], axis=0)
            ob = jnp.concatenate([ob[:, h * HD : (h + 1) * HD] for h in range(8)], axis=0)
            dv[kv_win, :] += jnp.dot(p_s[0:keys, :], ob, preferred_element_type=F32)
            dk[kv_win, :] += jnp.dot(ds_s[0:keys, :], qb, preferred_element_type=F32)
            dqt = lax.dot_general(
                kv_rows[kv_win, 0:HD], ds_s[0:keys, :], (((0,), (0,)), ((), ())), preferred_element_type=F32
            )
            for h in range(8):
                dq[pl.ds(pl.multiple_of(zb * ROWS, ROWS), ROWS), h * HD : (h + 1) * HD] = dqt[
                    :, h * HD : (h + 1) * HD
                ].T.astype(BF16)

    def attend(i, carry):
        d = jnp.where(i == 2, 3, jnp.where(i == 3, 2, i))
        zb = lax.rem(z + 4 - d, 4)
        lo, hi = jnp.where(i == 3, 0, 0), jnp.where(i == 3, 3, 0)

        with jax.named_scope("qowait"):

            @pl.when(d == 0)
            def _():
                own_q.wait()
                own_o.wait()

            @pl.when(d > 0)
            def _():
                remote(q_ref.at[:, 0:GW], qs.at[zb], qo_s.at[0, d], qo_r.at[0, d], core).wait_recv()
                remote(o_ref.at[:, 0:GW], os_.at[zb], qo_s.at[1, d], qo_r.at[1, d], core).wait_recv()

        @pl.when(i == 1)
        def _():
            own_w.wait()
            w_core.wait()

        with jax.named_scope("forward"):
            lax.fori_loop(lo, hi, forward_early, 0)
        block = zb * 4 + yc
        at = pl.multiple_of(block * ROWS, ROWS)

        @pl.when(zb > 0)
        def _():
            attend_block(zb, at, at, WIN)

        @pl.when(zb == 0)
        def _():
            attend_block(zb, at, 8 * ROWS, 4)

        with jax.named_scope("early"):
            lax.fori_loop(lo, hi, early, 0)
        return carry

    lax.fori_loop(0, 4, attend, 0)

    def blocks(b, carry):
        rows = pl.ds(pl.multiple_of((b * 2 + 1 - c + 8) * ROWS, ROWS), ROWS)
        at = lax.rem(b, 2)
        dkv_s[at, b // 2, :, 0:HD] = dk[rows, :].astype(BF16)
        dkv_s[at, b // 2, :, HD : 2 * HD] = dv[rows, :].astype(BF16)
        return carry

    lax.fori_loop(0, 8, blocks, 0)
    dkv_core = remote(dkv_s, dkv_c, dc_s.at[0], dc_r.at[0], core)
    dkv_core.start()

    def dd_y(i):
        return remote(dkv_o.at[1 - y], dkv_t, dd_s.at[0], dd_r.at[0], ypart)

    def dd_z(d):
        zz = zoff(d)
        return remote(dkv_p.at[zz], dkv_i.at[z], dd_s.at[d], dd_r.at[d], dev(zz, y, c))

    def product(n):
        cols = slice(n * CW, (n + 1) * CW)
        slot = n % SLOTS
        if n >= EARLY:
            with jax.named_scope("prodwait"):
                w_fwd_in(n).wait_recv()
        with jax.named_scope("proddot"):
            part[slot] = jnp.dot(dq[...], w_rows[:, cols], preferred_element_type=F32)
            own[:, cols] = part[slot, pl.ds(pl.multiple_of(z * ROWS, ROWS), ROWS), :]
            if n >= EARLY:
                for i in range(2):
                    half_s[i, n] = part[slot, far, i * (CW // 2) : (i + 1) * (CW // 2)].astype(BF16)
                for i in range(2):
                    half(i, n).start()

    def merge(n):
        slot = n % SLOTS
        for i in range(2):
            with jax.named_scope("mergewait"):
                half(i, n).wait_recv()
            rows = pl.ds(pl.multiple_of(zoff(1 if i == 0 else 3) * ROWS, ROWS), ROWS)
            mine = slice(0, CW // 2) if i == 0 else slice(CW // 2, CW)
            rest = slice(CW // 2, CW) if i == 0 else slice(0, CW // 2)
            full_s[i, n, :, mine] = (part[slot, rows, mine] + half_r[i, n].astype(F32)).astype(BF16)
            full_s[i, n, :, rest] = part[slot, rows, rest].astype(BF16)
            full(i, n).start()

    def hop(n):
        cols = pl.ds(n * CW, CW)
        return remote(fin.at[:, cols], out_ref.at[:, cols], hop_s.at[n], hop_r.at[n], (jnp.maximum(sec - 1, 0), seq))

    def finish(n):
        cols = slice(n * CW, (n + 1) * CW)
        with jax.named_scope("findot"):
            dkv = jnp.concatenate([dkv_i[zz] for zz in range(4)], axis=1)
            total = own[:, cols] + jnp.dot(dkv, wkv.reshape(GW, D)[:, cols], preferred_element_type=F32)
        with jax.named_scope("finwait"):
            full(0, n).wait_recv()
            full(1, n).wait_recv()
        total = total + full_r[0, n].astype(F32) + full_r[1, n].astype(F32)
        fin[:, cols] = total.astype(BF16)

        @pl.when(sec > 0)
        def _():
            hop(n).start()

    def dkv_core_sum():
        dkv_core.wait_recv()
        for yy in range(2):

            def add(zz, carry):
                rows = pl.ds(pl.multiple_of((zz * 4 + yy * 2 + c + 8) * ROWS, ROWS), ROWS)
                dkv_o[yy, zz, :, 0:HD] = (dk[rows, :] + dkv_c[yy, zz, :, 0:HD].astype(F32)).astype(BF16)
                dkv_o[yy, zz, :, HD : 2 * HD] = (dv[rows, :] + dkv_c[yy, zz, :, HD : 2 * HD].astype(F32)).astype(BF16)
                return carry

            lax.fori_loop(0, 4, add, 0)
        dd_y(0).start()
        for n in range(W_EARLY, NC):
            w_y(n).start()

    def dkv_y_sum():
        dd_y(0).wait_recv()

        def add(zz, carry):
            dkv_p[zz] = (dkv_o[y, zz].astype(F32) + dkv_t[zz].astype(F32)).astype(BF16)
            return carry

        lax.fori_loop(0, 4, add, 0)
        for d in (2, 1, 3):
            dd_z(d).start()
        dkv_i[z] = dkv_p[z]
        own_wk.wait()
        own_wv.wait()

    def dkv_arrived():
        for d in (2, 1, 3):
            zs = lax.rem(z + 4 - d, 4)
            remote(dkv_p.at[zs], dkv_i.at[zs], dd_s.at[d], dd_r.at[d], core).wait_recv()

    steps = {"p": product, "m": merge, "f": finish, "w": lambda n: forward(n, 0)}
    for step in ORDER:
        if step == "core":
            with jax.named_scope("dkvcore"):
                dkv_core_sum()
        elif step == "ysum":
            with jax.named_scope("ddywait"):
                dkv_y_sum()
        elif step == "dkv":
            with jax.named_scope("ddwait"):
                dkv_arrived()
        else:
            with jax.named_scope(step):
                steps[step[0]](int(step[1:]))

    @pl.when(sec == 7)
    def _():
        out_ref[...] = jnp.zeros_like(out_ref)

    with jax.named_scope("drain"):
        for pair in kv_copies:
            pair[0].wait_send()
            pair[1].wait_send()
        for d in range(4):
            kv_y(d).wait_send()
            kv_c(0, d).wait_send()
            kv_c(1, d).wait_send()
        for d in (1, 2, 3):
            for copy in qo_copies[d]:
                copy.wait_send()
        dkv_core.wait_send()
        dd_y(0).wait_send()
        for d in (1, 2, 3):
            dd_z(d).wait_send()

        def drain(n, carry):
            @pl.when(n > 0)
            def _():
                w_y(n).wait_send()

            w_fwd(n).wait_send()
            for i in range(2):
                half(i, n).wait_send()
                full(i, n).wait_send()

            @pl.when(sec > 0)
            def _():
                hop(n).wait_send()

            @pl.when(sec < 7)
            def _():
                hop(n).wait_recv()

            return carry

        w_y0(0).wait_send()
        w_y0(1).wait_send()
        lax.fori_loop(0, NC, drain, 0)


def body(queries, keys, values, out_grad, documents, query_weight, key_weight, value_weight):
    hbm = pl.BlockSpec(memory_space=pltpu.MemorySpace.HBM)
    vmem = pl.BlockSpec(memory_space=pltpu.VMEM)
    dma = pltpu.SemaphoreType.DMA
    scratch = [
        pltpu.VMEM((4, ROWS, GW), BF16),
        pltpu.VMEM((4, ROWS, GW), BF16),
        pltpu.VMEM((6, 4, ROWS, 2 * HD), BF16),
        pltpu.VMEM((1, 2048), jnp.int32),
        pltpu.VMEM((WIN * ROWS, GW), BF16),
        pltpu.VMEM((WIN * ROWS, GW), BF16),
        pltpu.VMEM((24 * ROWS, HD), F32),
        pltpu.VMEM((24 * ROWS, HD), F32),
        pltpu.VMEM((4 * ROWS, GW), BF16),
        pltpu.VMEM((4, 256, D), BF16),
        pltpu.VMEM((4, 2, HD, D), BF16),
        pltpu.VMEM((2, NC, ROWS, CW // 2), BF16),
        pltpu.VMEM((2, NC, ROWS, CW // 2), BF16),
        pltpu.VMEM((2, NC, ROWS, CW), BF16),
        pltpu.VMEM((2, NC, ROWS, CW), BF16),
        pltpu.VMEM((SLOTS, 4 * ROWS, CW), F32),
        pltpu.VMEM((ROWS, D), F32),
        pltpu.VMEM((2, 4, ROWS, 2 * HD), BF16),
        pltpu.VMEM((2, 4, ROWS, 2 * HD), BF16),
        pltpu.VMEM((2, 4, ROWS, 2 * HD), BF16),
        pltpu.VMEM((4, ROWS, 2 * HD), BF16),
        pltpu.VMEM((4, ROWS, 2 * HD), BF16),
        pltpu.VMEM((4, ROWS, 2 * HD), BF16),
        pltpu.VMEM((ROWS, D), BF16),
        dma((7,)),
        dma((2, 4)), dma((2, 4)),
        dma((4,)), dma((4,)),
        dma((2, 4)), dma((2, 4)),
        dma((2, 4)), dma((2, 4)),
        dma((2,)), dma((2,)),
        dma((NC,)), dma((NC,)),
        dma((1,)), dma((1,)),
        dma((NC,)), dma((NC,)),
        dma((2, NC)), dma((2, NC)),
        dma((2, NC)), dma((2, NC)),
        dma((1,)), dma((1,)),
        dma((4,)), dma((4,)),
        dma((NC,)), dma((NC,)),
    ]
    out = pl.pallas_call(
        kernel,
        out_shape=pltpu.VMEM((ROWS, D), BF16),
        in_specs=[hbm, hbm, hbm, hbm, vmem, hbm, hbm, hbm],
        out_specs=vmem,
        scratch_shapes=scratch,
        compiler_params=pltpu.CompilerParams(
            collective_id=0, has_side_effects=True, vmem_limit_bytes=62914560
        ),
    )(
        queries[0],
        keys[0],
        values[0],
        out_grad[0],
        documents,
        query_weight[0],
        key_weight[0].reshape(4, HD, D),
        value_weight[0].reshape(4, HD, D),
    )
    return out[None]


def solution(mesh):
    in_specs = (
        P("section", "seq", None),
        P("section", "seq", None),
        P("section", "seq", None),
        P("section", "seq", None),
        P("section", None),
        P("section", "seq", None),
        P("section", None, None),
        P("section", None, None),
    )
    out_specs = P("section", "seq", None)
    return jax.shard_map(body, mesh=mesh, in_specs=in_specs, out_specs=out_specs, check_vma=False)
```

```python
import math

import jax
import jax.numpy as jnp
from jax import lax
from jax.experimental import pallas as pl
from jax.experimental.pallas import tpu as pltpu
from jax.sharding import PartitionSpec as P

HD = 128
ROWS = 128
GW = 1024
D = 4096
NC = 8
CW = D // NC
W_EARLY = 7
EARLY = 3
SLOTS = 6
ORDER = (
    "w3", "core", "p0", "m0", "p3", "p1", "m1", "w4", "p4", "p2", "w5", "p5", "m2", "w6", "p6", "ysum", "m3",
    "m4", "dkv", "f0", "f1", "w7", "m5", "f2", "p7", "f3", "m6", "f4", "m7", "f5", "f6", "f7",
)
WIN = 9
SCALE = 1.0 / math.sqrt(HD)
NEG = -1e30
MESH = pl.DeviceIdType.MESH
F32 = jnp.float32
BF16 = jnp.bfloat16


def remote(src, dst, send, recv, device):
    return pltpu.make_async_remote_copy(
        src_ref=src, dst_ref=dst, send_sem=send, recv_sem=recv, device_id=device, device_id_type=MESH
    )


def kernel(
    q_ref, k_ref, v_ref, o_ref, doc_ref, w_ref, wk_ref, wv_ref,
    out_ref,
    qs, os_, kv, start, p_s, ds_s, dk, dv, dq, w8, wkv, half_s, half_r, full_s, full_r, part, own,
    dkv_s, dkv_c, dkv_o, dkv_t, dkv_p, dkv_i, fin,
    loc, kvz_s, kvz_r, kvy_s, kvy_r, kvc_s, kvc_r, qo_s, qo_r,
    w0_s, w0_r, wy_s, wy_r, wc_s, wc_r, wf_s, wf_r, ra_s, ra_r, rb_s, rb_r, dc_s, dc_r, dd_s, dd_r, hop_s, hop_r,
):
    sec = lax.axis_index("section")
    seq = lax.axis_index("seq")
    z = seq // 4
    y = lax.rem(seq // 2, 2)
    c = lax.rem(seq, 2)
    yc = y * 2 + c

    def dev(zz, yy, cc):
        return (sec, zz * 4 + yy * 2 + cc)

    def zoff(d):
        return lax.rem(z + d, 4)

    core = dev(z, y, 1 - c)
    ypart = dev(z, 1 - y, c)

    own_q = pltpu.make_async_copy(q_ref.at[:, pl.ds(pl.multiple_of(z * GW, GW), GW)], qs.at[z], loc.at[0])
    own_o = pltpu.make_async_copy(o_ref.at[:, pl.ds(pl.multiple_of(z * GW, GW), GW)], os_.at[z], loc.at[1])
    own_k = pltpu.make_async_copy(
        k_ref.at[:, pl.ds(pl.multiple_of(z * HD, HD), HD)], kv.at[z + 2, yc, :, 0:HD], loc.at[2]
    )
    own_v = pltpu.make_async_copy(
        v_ref.at[:, pl.ds(pl.multiple_of(z * HD, HD), HD)], kv.at[z + 2, yc, :, HD : 2 * HD], loc.at[3]
    )
    own_w = pltpu.make_async_copy(w_ref, w8.at[yc], loc.at[4])
    own_wk = pltpu.make_async_copy(wk_ref, wkv.at[:, 0], loc.at[5])
    own_wv = pltpu.make_async_copy(wv_ref, wkv.at[:, 1], loc.at[6])
    barrier = pltpu.get_barrier_semaphore()
    for partner in (dev(zoff(1), y, c), dev(zoff(2), y, c), dev(zoff(3), y, c), ypart, core):
        pl.semaphore_signal(barrier, inc=1, device_id=partner, device_id_type=MESH)

    @pl.when(sec > 0)
    def _():
        pl.semaphore_signal(barrier, inc=1, device_id=(sec - 1, seq), device_id_type=MESH)

    @pl.when(sec < 7)
    def _():
        pl.semaphore_signal(barrier, inc=1, device_id=(sec + 1, seq), device_id_type=MESH)

    for copy in (own_k, own_v, own_q, own_o, own_w, own_wk, own_wv):
        copy.start()
    doc = doc_ref[...]
    first = jnp.zeros_like(doc)
    for value in (1, 2, 3):
        before = jnp.sum((doc < value).astype(F32), axis=1, keepdims=True).astype(jnp.int32)
        first = jnp.where(doc == value, before, first)
    start[...] = first
    kv[0:2] = jnp.zeros((2, 4, ROWS, 2 * HD), BF16)
    dk[...] = jnp.zeros_like(dk)
    dv[...] = jnp.zeros_like(dv)
    own_k.wait()
    own_v.wait()
    with jax.named_scope("barrier"):
        pl.semaphore_wait(barrier, 5 + jnp.where(sec > 0, 1, 0) + jnp.where(sec < 7, 1, 0))

    kv_copies = []
    for d in (1, 3, 2):
        zd = zoff(d)
        cols = pl.ds(pl.multiple_of(zd * HD, HD), HD)
        kv_copies.append(
            (
                remote(k_ref.at[:, cols], kv.at[z + 2, yc, :, 0:HD], kvz_s.at[0, d], kvz_r.at[0, d], dev(zd, y, c)),
                remote(
                    v_ref.at[:, cols], kv.at[z + 2, yc, :, HD : 2 * HD], kvz_s.at[1, d], kvz_r.at[1, d], dev(zd, y, c)
                ),
            )
        )
    for pair in kv_copies:
        pair[0].start()
        pair[1].start()

    def kv_y(d):
        zs = lax.rem(z + 4 - d, 4) + 2
        return remote(kv.at[zs, yc], kv.at[zs, yc], kvy_s.at[d], kvy_r.at[d], ypart)

    def kv_y_in(d):
        zs = lax.rem(z + 4 - d, 4) + 2
        at = (1 - y) * 2 + c
        return remote(kv.at[zs, at], kv.at[zs, at], kvy_s.at[d], kvy_r.at[d], ypart)

    def kv_c(i, d):
        zs = lax.rem(z + 4 - d, 4) + 2
        at = yc if i == 0 else (1 - y) * 2 + c
        return remote(kv.at[zs, at], kv.at[zs, at], kvc_s.at[i, d], kvc_r.at[i, d], core)

    def kv_c_in(i, d):
        zs = lax.rem(z + 4 - d, 4) + 2
        at = (y if i == 0 else 1 - y) * 2 + 1 - c
        return remote(kv.at[zs, at], kv.at[zs, at], kvc_s.at[i, d], kvc_r.at[i, d], core)

    def w_y0(i):
        cols = pl.ds(i * (CW // 2), CW // 2)
        return remote(w_ref.at[:, cols], w8.at[yc, :, cols], w0_s.at[i], w0_r.at[i], ypart)

    def w_y0_in(i):
        cols = pl.ds(i * (CW // 2), CW // 2)
        at = (1 - y) * 2 + c
        return remote(w_ref.at[:, cols], w8.at[at, :, cols], w0_s.at[i], w0_r.at[i], ypart)

    def w_y(n):
        cols = pl.ds(n * CW, CW)
        return remote(w_ref.at[:, cols], w8.at[yc, :, cols], wy_s.at[n], wy_r.at[n], ypart)

    def w_y_in(n):
        cols = pl.ds(n * CW, CW)
        at = (1 - y) * 2 + c
        return remote(w_ref.at[:, cols], w8.at[at, :, cols], wy_s.at[n], wy_r.at[n], ypart)

    w_core = remote(w_ref, w8.at[yc], wc_s.at[0], wc_r.at[0], core)

    def w_fwd(n):
        cols = pl.ds(n * CW, CW)
        at = (1 - y) * 2 + c
        return remote(w8.at[at, :, cols], w8.at[at, :, cols], wf_s.at[n], wf_r.at[n], core)

    def w_fwd_in(n):
        cols = pl.ds(n * CW, CW)
        at = (1 - y) * 2 + 1 - c
        return remote(w8.at[at, :, cols], w8.at[at, :, cols], wf_s.at[n], wf_r.at[n], core)

    qo_copies = {}
    for d in (1, 3, 2):
        zd = zoff(d)
        cols = pl.ds(pl.multiple_of(zd * GW, GW), GW)
        qo_copies[d] = (
            remote(q_ref.at[:, cols], qs.at[z], qo_s.at[0, d], qo_r.at[0, d], dev(zd, y, c)),
            remote(o_ref.at[:, cols], os_.at[z], qo_s.at[1, d], qo_r.at[1, d], dev(zd, y, c)),
        )

    kv_y(0).start()
    kv_c(0, 0).start()
    w_y0(0).start()
    with jax.named_scope("kvz"):
        for d in (1, 3, 2):
            zs = lax.rem(z + 4 - d, 4)
            remote(k_ref.at[:, 0:HD], kv.at[zs + 2, yc, :, 0:HD], kvz_s.at[0, d], kvz_r.at[0, d], core).wait_recv()
            remote(
                v_ref.at[:, 0:HD], kv.at[zs + 2, yc, :, HD : 2 * HD], kvz_s.at[1, d], kvz_r.at[1, d], core
            ).wait_recv()
            kv_y(d).start()
            kv_c(0, d).start()
    for d in (1, 3, 2):
        for copy in qo_copies[d]:
            copy.start()
    w_y0(1).start()
    for n in range(1, W_EARLY):
        w_y(n).start()
    with jax.named_scope("kvy"):
        for d in (0, 1, 3, 2):
            kv_y_in(d).wait_recv()
            kv_c(1, d).start()
    w_core.start()
    with jax.named_scope("kvc"):
        for i in range(2):
            for d in range(4):
                kv_c_in(i, d).wait_recv()

    kv_rows = kv.reshape(24 * ROWS, 2 * HD)
    w_rows = w8.reshape(GW, D)
    up, down = dev(zoff(1), y, c), dev(zoff(3), y, c)
    far = pl.ds(pl.multiple_of(zoff(2) * ROWS, ROWS), ROWS)

    def half(i, n):
        return remote(half_s.at[i, n], half_r.at[i, n], ra_s.at[i, n], ra_r.at[i, n], up if i == 0 else down)

    def full(i, n):
        return remote(full_s.at[i, n], full_r.at[i, n], rb_s.at[i, n], rb_r.at[i, n], up if i == 0 else down)

    def forward(n, carry):
        w_y_in(n).wait_recv()
        w_fwd(n).start()
        return carry

    def forward_early(n, carry):
        @pl.when(n == 0)
        def _():
            w_y0_in(0).wait_recv()
            w_y0_in(1).wait_recv()

        @pl.when(n > 0)
        def _():
            w_y_in(n).wait_recv()

        w_fwd(n).start()
        return carry

    def early(n, carry):
        cols = pl.ds(pl.multiple_of(n * CW, CW), CW)
        w_fwd_in(n).wait_recv()
        res = jnp.dot(dq[far, :], w_rows[:, cols], preferred_element_type=F32).astype(BF16)
        for i in range(2):
            half_s[i, n] = res[:, i * (CW // 2) : (i + 1) * (CW // 2)]
            half(i, n).start()
        return carry

    def attend_block(zb, at, key_at, win):
        keys = win * ROWS
        base = at - 8 * ROWS if win == WIN else 0
        lower = start[:, pl.ds(at, ROWS)] - base
        lower = jnp.concatenate([lower, lower], axis=1)
        kv_win = pl.ds(key_at, keys)

        def heads(hp, carry):
            cols = pl.ds(pl.multiple_of(hp * 2 * HD, 2 * HD), 2 * HD)
            q2 = qs[zb, :, cols]
            q2 = jnp.concatenate([q2[:, 0:HD], q2[:, HD:]], axis=0)
            o2 = os_[zb, :, cols]
            o2 = jnp.concatenate([o2[:, 0:HD], o2[:, HD:]], axis=0)
            v_win = kv_rows[kv_win, HD : 2 * HD]
            k_win = kv_rows[kv_win, 0:HD]
            nt = (((1,), (1,)), ((), ()))
            s = lax.dot_general(k_win, q2, nt, preferred_element_type=F32)
            free = 8 * ROWS if win == WIN else 0
            rest = keys - free
            key = lax.broadcasted_iota(jnp.int32, (rest, 2 * ROWS), 0) + free
            row = lax.broadcasted_iota(jnp.int32, (rest, 2 * ROWS), 1)
            row = jnp.where(row >= ROWS, row - ROWS, row) + (free if win == WIN else yc * ROWS)
            s_b = jnp.where((key >= lower) & (key <= row), s[free:], NEG)
            if free:
                key = lax.broadcasted_iota(jnp.int32, (free, 2 * ROWS), 0)
                s_b = jnp.concatenate([jnp.where(key >= lower, s[:free], NEG), s_b], axis=0)
            s = s_b
            top = jnp.max(s, axis=0, keepdims=True)
            e = jnp.exp2((s - top) * (SCALE * math.log2(math.e)))
            inv = 1.0 / jnp.sum(e, axis=0, keepdims=True)
            dp = lax.dot_general(v_win, o2, nt, preferred_element_type=F32)
            delta = jnp.sum(e * dp, axis=0, keepdims=True) * inv
            p_s[0:keys, cols] = (e * inv).astype(BF16)
            ds_s[0:keys, cols] = (e * (dp - delta) * (inv * SCALE)).astype(BF16)
            return carry

        with jax.named_scope("heads"):
            lax.fori_loop(0, 4, heads, 0, unroll=4)
        with jax.named_scope("grads"):
            qb = qs[zb]
            ob = os_[zb]
            qb = jnp.concatenate([qb[:, h * HD : (h + 1) * HD] for h in range(8)], axis=0)
            ob = jnp.concatenate([ob[:, h * HD : (h + 1) * HD] for h in range(8)], axis=0)
            dv[kv_win, :] += jnp.dot(p_s[0:keys, :], ob, preferred_element_type=F32)
            dk[kv_win, :] += jnp.dot(ds_s[0:keys, :], qb, preferred_element_type=F32)
            dqt = lax.dot_general(
                kv_rows[kv_win, 0:HD], ds_s[0:keys, :], (((0,), (0,)), ((), ())), preferred_element_type=F32
            )
            for h in range(8):
                dq[pl.ds(pl.multiple_of(zb * ROWS, ROWS), ROWS), h * HD : (h + 1) * HD] = dqt[
                    :, h * HD : (h + 1) * HD
                ].T.astype(BF16)

    def attend(i, carry):
        d = jnp.where(i == 2, 3, jnp.where(i == 3, 2, i))
        zb = lax.rem(z + 4 - d, 4)
        lo, hi = jnp.where(i == 3, 0, 0), jnp.where(i == 3, 3, 0)

        with jax.named_scope("qowait"):

            @pl.when(d == 0)
            def _():
                own_q.wait()
                own_o.wait()

            @pl.when(d > 0)
            def _():
                remote(q_ref.at[:, 0:GW], qs.at[zb], qo_s.at[0, d], qo_r.at[0, d], core).wait_recv()
                remote(o_ref.at[:, 0:GW], os_.at[zb], qo_s.at[1, d], qo_r.at[1, d], core).wait_recv()

        @pl.when(i == 1)
        def _():
            own_w.wait()
            w_core.wait()

        with jax.named_scope("forward"):
            lax.fori_loop(lo, hi, forward_early, 0)
        block = zb * 4 + yc
        at = pl.multiple_of(block * ROWS, ROWS)

        @pl.when(zb > 0)
        def _():
            attend_block(zb, at, at, WIN)

        @pl.when(zb == 0)
        def _():
            attend_block(zb, at, 8 * ROWS, 4)

        with jax.named_scope("early"):
            lax.fori_loop(lo, hi, early, 0)
        return carry

    lax.fori_loop(0, 4, attend, 0)

    def blocks(b, carry):
        rows = pl.ds(pl.multiple_of((b * 2 + 1 - c + 8) * ROWS, ROWS), ROWS)
        at = lax.rem(b, 2)
        dkv_s[at, b // 2, :, 0:HD] = dk[rows, :].astype(BF16)
        dkv_s[at, b // 2, :, HD : 2 * HD] = dv[rows, :].astype(BF16)
        return carry

    lax.fori_loop(0, 8, blocks, 0)
    dkv_core = remote(dkv_s, dkv_c, dc_s.at[0], dc_r.at[0], core)
    dkv_core.start()

    def dd_y(i):
        return remote(dkv_o.at[1 - y], dkv_t, dd_s.at[0], dd_r.at[0], ypart)

    def dd_z(d):
        zz = zoff(d)
        return remote(dkv_p.at[zz], dkv_i.at[z], dd_s.at[d], dd_r.at[d], dev(zz, y, c))

    def product(n):
        cols = slice(n * CW, (n + 1) * CW)
        slot = n % SLOTS
        if n >= EARLY:
            with jax.named_scope("prodwait"):
                w_fwd_in(n).wait_recv()
        with jax.named_scope("proddot"):
            part[slot] = jnp.dot(dq[...], w_rows[:, cols], preferred_element_type=F32)
            own[:, cols] = part[slot, pl.ds(pl.multiple_of(z * ROWS, ROWS), ROWS), :]
            if n >= EARLY:
                for i in range(2):
                    half_s[i, n] = part[slot, far, i * (CW // 2) : (i + 1) * (CW // 2)].astype(BF16)
                for i in range(2):
                    half(i, n).start()

    def merge(n):
        slot = n % SLOTS
        for i in range(2):
            with jax.named_scope("mergewait"):
                half(i, n).wait_recv()
            rows = pl.ds(pl.multiple_of(zoff(1 if i == 0 else 3) * ROWS, ROWS), ROWS)
            mine = slice(0, CW // 2) if i == 0 else slice(CW // 2, CW)
            rest = slice(CW // 2, CW) if i == 0 else slice(0, CW // 2)
            full_s[i, n, :, mine] = (part[slot, rows, mine] + half_r[i, n].astype(F32)).astype(BF16)
            full_s[i, n, :, rest] = part[slot, rows, rest].astype(BF16)
            full(i, n).start()

    def hop(n):
        cols = pl.ds(n * CW, CW)
        return remote(fin.at[:, cols], out_ref.at[:, cols], hop_s.at[n], hop_r.at[n], (jnp.maximum(sec - 1, 0), seq))

    def finish(n):
        cols = slice(n * CW, (n + 1) * CW)
        with jax.named_scope("findot"):
            dkv = jnp.concatenate([dkv_i[zz] for zz in range(4)], axis=1)
            total = own[:, cols] + jnp.dot(dkv, wkv.reshape(GW, D)[:, cols], preferred_element_type=F32)
        with jax.named_scope("finwait"):
            full(0, n).wait_recv()
            full(1, n).wait_recv()
        total = total + full_r[0, n].astype(F32) + full_r[1, n].astype(F32)
        fin[:, cols] = total.astype(BF16)

        @pl.when(sec > 0)
        def _():
            hop(n).start()

    def dkv_core_sum():
        dkv_core.wait_recv()
        for yy in range(2):

            def add(zz, carry):
                rows = pl.ds(pl.multiple_of((zz * 4 + yy * 2 + c + 8) * ROWS, ROWS), ROWS)
                dkv_o[yy, zz, :, 0:HD] = (dk[rows, :] + dkv_c[yy, zz, :, 0:HD].astype(F32)).astype(BF16)
                dkv_o[yy, zz, :, HD : 2 * HD] = (dv[rows, :] + dkv_c[yy, zz, :, HD : 2 * HD].astype(F32)).astype(BF16)
                return carry

            lax.fori_loop(0, 4, add, 0)
        dd_y(0).start()
        for n in range(W_EARLY, NC):
            w_y(n).start()

    def dkv_y_sum():
        dd_y(0).wait_recv()

        def add(zz, carry):
            dkv_p[zz] = (dkv_o[y, zz].astype(F32) + dkv_t[zz].astype(F32)).astype(BF16)
            return carry

        lax.fori_loop(0, 4, add, 0)
        for d in (2, 1, 3):
            dd_z(d).start()
        dkv_i[z] = dkv_p[z]
        own_wk.wait()
        own_wv.wait()

    def dkv_arrived():
        for d in (2, 1, 3):
            zs = lax.rem(z + 4 - d, 4)
            remote(dkv_p.at[zs], dkv_i.at[zs], dd_s.at[d], dd_r.at[d], core).wait_recv()

    steps = {"p": product, "m": merge, "f": finish, "w": lambda n: forward(n, 0)}
    for step in ORDER:
        if step == "core":
            with jax.named_scope("dkvcore"):
                dkv_core_sum()
        elif step == "ysum":
            with jax.named_scope("ddywait"):
                dkv_y_sum()
        elif step == "dkv":
            with jax.named_scope("ddwait"):
                dkv_arrived()
        else:
            with jax.named_scope(step):
                steps[step[0]](int(step[1:]))

    @pl.when(sec == 7)
    def _():
        out_ref[...] = jnp.zeros_like(out_ref)

    with jax.named_scope("drain"):
        for pair in kv_copies:
            pair[0].wait_send()
            pair[1].wait_send()
        for d in range(4):
            kv_y(d).wait_send()
            kv_c(0, d).wait_send()
            kv_c(1, d).wait_send()
        for d in (1, 2, 3):
            for copy in qo_copies[d]:
                copy.wait_send()
        dkv_core.wait_send()
        dd_y(0).wait_send()
        for d in (1, 2, 3):
            dd_z(d).wait_send()

        def drain(n, carry):
            @pl.when(n > 0)
            def _():
                w_y(n).wait_send()

            w_fwd(n).wait_send()
            for i in range(2):
                half(i, n).wait_send()
                full(i, n).wait_send()

            @pl.when(sec > 0)
            def _():
                hop(n).wait_send()

            @pl.when(sec < 7)
            def _():
                hop(n).wait_recv()

            return carry

        w_y0(0).wait_send()
        w_y0(1).wait_send()
        lax.fori_loop(0, NC, drain, 0)


def body(queries, keys, values, out_grad, documents, query_weight, key_weight, value_weight):
    hbm = pl.BlockSpec(memory_space=pltpu.MemorySpace.HBM)
    vmem = pl.BlockSpec(memory_space=pltpu.VMEM)
    dma = pltpu.SemaphoreType.DMA
    scratch = [
        pltpu.VMEM((4, ROWS, GW), BF16),
        pltpu.VMEM((4, ROWS, GW), BF16),
        pltpu.VMEM((6, 4, ROWS, 2 * HD), BF16),
        pltpu.VMEM((1, 2048), jnp.int32),
        pltpu.VMEM((WIN * ROWS, GW), BF16),
        pltpu.VMEM((WIN * ROWS, GW), BF16),
        pltpu.VMEM((24 * ROWS, HD), F32),
        pltpu.VMEM((24 * ROWS, HD), F32),
        pltpu.VMEM((4 * ROWS, GW), BF16),
        pltpu.VMEM((4, 256, D), BF16),
        pltpu.VMEM((4, 2, HD, D), BF16),
        pltpu.VMEM((2, NC, ROWS, CW // 2), BF16),
        pltpu.VMEM((2, NC, ROWS, CW // 2), BF16),
        pltpu.VMEM((2, NC, ROWS, CW), BF16),
        pltpu.VMEM((2, NC, ROWS, CW), BF16),
        pltpu.VMEM((SLOTS, 4 * ROWS, CW), F32),
        pltpu.VMEM((ROWS, D), F32),
        pltpu.VMEM((2, 4, ROWS, 2 * HD), BF16),
        pltpu.VMEM((2, 4, ROWS, 2 * HD), BF16),
        pltpu.VMEM((2, 4, ROWS, 2 * HD), BF16),
        pltpu.VMEM((4, ROWS, 2 * HD), BF16),
        pltpu.VMEM((4, ROWS, 2 * HD), BF16),
        pltpu.VMEM((4, ROWS, 2 * HD), BF16),
        pltpu.VMEM((ROWS, D), BF16),
        dma((7,)),
        dma((2, 4)), dma((2, 4)),
        dma((4,)), dma((4,)),
        dma((2, 4)), dma((2, 4)),
        dma((2, 4)), dma((2, 4)),
        dma((2,)), dma((2,)),
        dma((NC,)), dma((NC,)),
        dma((1,)), dma((1,)),
        dma((NC,)), dma((NC,)),
        dma((2, NC)), dma((2, NC)),
        dma((2, NC)), dma((2, NC)),
        dma((1,)), dma((1,)),
        dma((4,)), dma((4,)),
        dma((NC,)), dma((NC,)),
    ]
    out = pl.pallas_call(
        kernel,
        out_shape=pltpu.VMEM((ROWS, D), BF16),
        in_specs=[hbm, hbm, hbm, hbm, vmem, hbm, hbm, hbm],
        out_specs=vmem,
        scratch_shapes=scratch,
        compiler_params=pltpu.CompilerParams(
            collective_id=0, has_side_effects=True, vmem_limit_bytes=62914560
        ),
    )(
        queries[0],
        keys[0],
        values[0],
        out_grad[0],
        documents,
        query_weight[0],
        key_weight[0].reshape(4, HD, D),
        value_weight[0].reshape(4, HD, D),
    )
    return out[None]


def solution(mesh):
    in_specs = (
        P("section", "seq", None),
        P("section", "seq", None),
        P("section", "seq", None),
        P("section", "seq", None),
        P("section", None),
        P("section", "seq", None),
        P("section", None, None),
        P("section", None, None),
    )
    out_specs = P("section", "seq", None)
    return jax.shard_map(body, mesh=mesh, in_specs=in_specs, out_specs=out_specs, check_vma=False)
```
